32 devices in a mesh: tm: 4 (over x, core), batch: 8 (over z, y).
Axes of the slice: x: 2, y: 2, z: 4, core: 2. Of those that a mesh axis runs over, the one named last changes fastest.
Arguments:
- latents: float32 [8, 16, 4096], P('tm', None, 'batch'), may hold values from -6 to 6
- shifts: int32 [16], replicated, may hold values from 0 to 7
- starts: int32 [16], replicated, may hold values from 0 to 2
- labels: int32 [16], replicated, may hold values from 0 to 1000
- class_table: bfloat16 [1001, 1152], replicated, may hold values from -6 to 6
- w_freq: bfloat16 [256, 1152], replicated, may hold values from -0.375 to 0.375
- w_time: bfloat16 [1152, 1152], replicated, may hold values from -0.1875 to 0.1875
- w_ada: bfloat16 [1152, 9216], P(None, 'tm'), may hold values from -0.1875 to 0.1875
- w_patch: bfloat16 [16, 1152], replicated, may hold values from -1.5 to 1.5
- w_qkv: bfloat16 [1152, 3456], P('batch', 'tm'), may hold values from -1 to 1
- w_proj: bfloat16 [1152, 1152], P('tm', 'batch'), may hold values from -0.1875 to 0.1875
- w_fc1: bfloat16 [1152, 4608], P('batch', 'tm'), may hold values from -0.1875 to 0.1875
- w_fc2: bfloat16 [4608, 1152], P('tm', 'batch'), may hold values from -0.09375 to 0.09375
- w_final: bfloat16 [1152, 16], replicated, may hold values from -0.1875 to 0.1875
Outputs:
- new_latents: float32 [8, 16, 4096], P('tm', None, 'batch')
- velocity: bfloat16 [8, 16, 4096], P('tm', None, 'batch')
The draws below stay inside these ranges and needn't reach their ends.
All inputs are finite; a program needn't handle non-finite values.
Results may differ from the reference program's by a relative error of at most 0.0091.
Values may be sent and summed in bfloat16 or wider, within the bound.
A program may use at most 128 MiB of HBM per device.

```python
import math
import jax
import jax.numpy as jnp
from jax import lax

D = 1152
HEADS = 16
FF = 4608
FREQ = 256
NCLASS = 1001
GRID = 16
WIN = 8
STEPS = 18
BATCH = 16
LAT = 4096


def draw_w_qkv(key, part):
    base_key = jax.random.fold_in(key, 0)
    head_size = D // HEADS
    base = jax.random.truncated_normal(base_key, -6.0, 6.0, (D, HEADS, 3, head_size), jnp.float32) / math.sqrt(D)
    return jnp.clip(base, -1.0, 1.0).reshape(D, 3 * D).astype(jnp.bfloat16)


def set_ends(entries, own_key, smallest, high):
    longest = entries.shape.index(max(entries.shape))
    spots = []
    for shift in (0, 1):
        where = [jax.random.randint(jax.random.fold_in(own_key, axis), (), 0, length) for axis, length in enumerate(entries.shape)]
        where[longest] = (where[longest] + shift) % entries.shape[longest]
        spots.append(tuple(where))
    return entries.at[spots[0]].set(smallest).at[spots[1]].set(high)


def block_levels(key, shape, shards, low, top_value):
    factor_of = 1.0
    for dim, blocks in shards:
        steps = jax.random.uniform(jax.random.fold_in(jax.random.fold_in(key, 6), dim), (blocks,), jnp.float32, low / len(shards), top_value / len(shards))
        factor_of = factor_of * jnp.repeat(jnp.exp(steps), shape[dim] // blocks).reshape((-1,) + (1,) * (len(shape) - 1 - dim))
    return factor_of


def gaussian(key, shape, deviation, bound, shards=(), held_as=jnp.bfloat16):
    loudness = block_levels(key, shape, shards, -0.22, 0.18) if shards else 1.0
    entries = jax.random.normal(key, shape, jnp.float32) * deviation * loudness
    return jnp.minimum(jnp.maximum(entries, -bound), bound).astype(held_as)


def setup_inputs(seed: int = 0) -> dict:
    arg_keys = jax.random.split(jax.random.key(seed), 15)
    latents = gaussian(arg_keys[0], (WIN, BATCH, LAT), 1.0, 6.0, ((0, 4), (2, 8)), jnp.float32)
    shifts = set_ends(jax.random.randint(arg_keys[1], (BATCH,), 0, WIN), jax.random.fold_in(arg_keys[1], 1), 0, WIN - 1).astype(jnp.int32)
    starts = set_ends(jax.random.randint(arg_keys[2], (BATCH,), 0, STEPS - 2 * WIN + 1), jax.random.fold_in(arg_keys[2], 1), 0, STEPS - 2 * WIN).astype(jnp.int32)
    labels = set_ends(jax.random.randint(arg_keys[3], (BATCH,), 0, NCLASS), jax.random.fold_in(arg_keys[3], 1), 0, NCLASS - 1).astype(jnp.int32)
    class_table = gaussian(arg_keys[4], (NCLASS, D), 1.0, 6.0)
    w_freq = gaussian(arg_keys[5], (FREQ, D), FREQ ** -0.5, 0.375)
    w_time = gaussian(arg_keys[6], (D, D), D ** -0.5, 0.1875)
    w_ada = gaussian(arg_keys[7], (D, 8 * D), D ** -0.5, 0.1875, ((1, 4),))
    w_patch = gaussian(arg_keys[8], (16, D), 16 ** -0.5, 1.5)
    w_qkv = draw_w_qkv(jax.random.fold_in(arg_keys[14], 71), 0)
    w_proj = gaussian(arg_keys[10], (D, D), D ** -0.5, 0.1875, ((0, 4), (1, 8)))
    w_fc1 = gaussian(arg_keys[11], (D, FF), D ** -0.5, 0.1875, ((0, 8), (1, 4)))
    w_fc2 = gaussian(arg_keys[12], (FF, D), FF ** -0.5, 0.09375, ((0, 4), (1, 8)))
    w_final = gaussian(arg_keys[13], (D, 16), D ** -0.5, 0.1875)
    return dict(latents=latents, shifts=shifts, starts=starts, labels=labels, class_table=class_table, w_freq=w_freq, w_time=w_time, w_ada=w_ada, w_patch=w_patch, w_qkv=w_qkv, w_proj=w_proj, w_fc1=w_fc1, w_fc2=w_fc2, w_final=w_final)


def layer_norm(values):
    average = lax.optimization_barrier(jnp.mean(values, axis=-1, keepdims=True))
    centred = values - average
    variance = lax.optimization_barrier(jnp.mean(centred * centred, axis=-1, keepdims=True))
    return centred * lax.rsqrt(variance + 1e-06)

def position_table(token_count):
    token_ids = jnp.arange(token_count, dtype=jnp.int32)
    row_ids = (token_ids // GRID).astype(jnp.float32)
    col_ids = (token_ids % GRID).astype(jnp.float32)
    quarter = D // 4
    omegas = jnp.exp(-math.log(10000.0) * jnp.arange(quarter, dtype=jnp.float32) / quarter)
    col_angle = col_ids[:, None] * omegas[None, :]
    row_angle = row_ids[:, None] * omegas[None, :]
    return jnp.concatenate([jnp.sin(col_angle), jnp.cos(col_angle), jnp.sin(row_angle), jnp.cos(row_angle)], axis=1)

def cond_activation(step_ids, class_ids, class_table, w_freq, w_time):
    half_freq = FREQ // 2
    freqs = jnp.exp(-math.log(10000.0) * jnp.arange(half_freq, dtype=jnp.float32) / half_freq)
    tvalue = 1000.0 * (1.0 - step_ids.astype(jnp.float32) / STEPS)
    angles = tvalue[:, None] * freqs[None, :]
    embedded = jnp.concatenate([jnp.cos(angles), jnp.sin(angles)], axis=1).astype(jnp.bfloat16)
    hidden_time = jax.nn.silu(jnp.dot(embedded, w_freq, preferred_element_type=jnp.float32)).astype(jnp.bfloat16)
    condition = jnp.dot(hidden_time, w_time, preferred_element_type=jnp.float32) + jnp.take(class_table, class_ids, axis=0).astype(jnp.float32)
    return jax.nn.silu(condition).astype(jnp.bfloat16)

def attend(qkv_rows):
    token_count = qkv_rows.shape[0]
    head_size = D // HEADS
    grouped = qkv_rows.reshape(token_count, HEADS, 3, head_size)
    query = grouped[:, :, 0, :].astype(jnp.float32)
    keys = grouped[:, :, 1, :].astype(jnp.float32)
    values = grouped[:, :, 2, :].astype(jnp.float32)
    scores = jnp.einsum('qhd,khd->hqk', query, keys) * (1.0 / math.sqrt(head_size))
    peak = lax.optimization_barrier(jnp.max(scores, axis=-1, keepdims=True))
    weights = jnp.exp(scores - peak)
    weights = weights / lax.optimization_barrier(jnp.sum(weights, axis=-1, keepdims=True))
    rounded = lax.optimization_barrier(weights.astype(jnp.bfloat16))
    attended = jnp.einsum('hqk,khd->qhd', rounded.astype(jnp.float32), values)
    return attended.astype(jnp.bfloat16).reshape(token_count, HEADS * head_size)

def denoise(point_row, modulation, w_patch, w_qkv, w_proj, w_fc1, w_fc2, w_final):
    patch_size = w_patch.shape[0]
    token_count = point_row.shape[0] // patch_size
    patch_in = point_row.reshape(token_count, patch_size).astype(jnp.bfloat16)
    tokens = jnp.dot(patch_in, w_patch, preferred_element_type=jnp.float32) + position_table(token_count)
    mod_float = modulation.astype(jnp.float32)
    mod_parts = [mod_float[block_index * D:(block_index + 1) * D][None, :] for block_index in range(8)]
    normed = (layer_norm(tokens) * (1.0 + mod_parts[1]) + mod_parts[0]).astype(jnp.bfloat16)
    qkv_rows = jnp.dot(normed, w_qkv, preferred_element_type=jnp.float32).astype(jnp.bfloat16)
    attended = attend(qkv_rows)
    mixed = tokens + mod_parts[2] * jnp.dot(attended, w_proj, preferred_element_type=jnp.float32)
    normed_two = (layer_norm(mixed) * (1.0 + mod_parts[4]) + mod_parts[3]).astype(jnp.bfloat16)
    hidden_units = jax.nn.gelu(jnp.dot(normed_two, w_fc1, preferred_element_type=jnp.float32), approximate=True).astype(jnp.bfloat16)
    residual = mixed + mod_parts[5] * jnp.dot(hidden_units, w_fc2, preferred_element_type=jnp.float32)
    final_in = (layer_norm(residual) * (1.0 + mod_parts[7]) + mod_parts[6]).astype(jnp.bfloat16)
    return jnp.dot(final_in, w_final, preferred_element_type=jnp.float32).astype(jnp.bfloat16).reshape(-1)

def reference(latents, shifts, starts, labels, class_table, w_freq, w_time, w_ada, w_patch, w_qkv, w_proj, w_fc1, w_fc2, w_final):
    positions = jnp.arange(WIN, dtype=jnp.int32)[:, None]
    source_rows = jnp.minimum(positions + shifts[None, :], WIN - 1).astype(jnp.int32)
    points = jnp.take_along_axis(latents, source_rows[:, :, None], axis=0)
    step_ids = (starts + shifts)[None, :] + positions
    class_ids = jnp.broadcast_to(labels[None, :], (WIN, BATCH))
    activation = cond_activation(step_ids.reshape(-1), class_ids.reshape(-1), class_table, w_freq, w_time)
    modulation = jnp.dot(activation, w_ada, preferred_element_type=jnp.float32).astype(jnp.bfloat16)

    def one_point(paired):
        return denoise(paired[0], paired[1], w_patch, w_qkv, w_proj, w_fc1, w_fc2, w_final)
    velocity = lax.map(one_point, (points.reshape(WIN * BATCH, LAT), modulation)).reshape(WIN, BATCH, LAT)
    velocity_float = velocity.astype(jnp.float32)
    summed = jnp.cumsum(velocity_float, axis=0)
    running = jnp.concatenate([jnp.zeros_like(summed[:1]), summed[:-1]], axis=0)
    new_latents = points[0][None] + running * (1.0 / STEPS)
    return (new_latents, velocity)
```

```python
import functools
import math

import jax
import jax.numpy as jnp
import numpy as np
from jax import lax
from jax.experimental import pallas as pl
from jax.experimental.pallas import tpu as pltpu
from jax.sharding import PartitionSpec as P

D = 1152
HEADS = 16
FREQ = 256
GRID = 16
STEPS = 18
LANES = 128
CORES = 2
MESH = pl.DeviceIdType.MESH


def entering(part, axis, combine, identity):
    place = lax.axis_index(axis)
    gathered = lax.all_gather(part, axis)
    state = jnp.zeros_like(part) + jnp.asarray(identity, part.dtype)

    def one(lap, state):
        return combine(state, lax.dynamic_index_in_dim(gathered, lap, 0, False))

    return lax.fori_loop(0, place, one, state)


def layer_norm(values):
    average = jnp.mean(values, axis=-1, keepdims=True)
    centred = values - average
    variance = jnp.mean(centred * centred, axis=-1, keepdims=True)
    return centred * lax.rsqrt(variance + 1e-06)


def position_table(token_count, group):
    token_ids = np.arange(token_count).reshape(token_count // group, group).T.reshape(-1)
    row_ids = (token_ids // GRID).astype(np.float32)
    col_ids = (token_ids % GRID).astype(np.float32)
    quarter = D // 4
    omegas = np.exp(-math.log(10000.0) * np.arange(quarter, dtype=np.float32) / quarter).astype(np.float32)
    col_angle = col_ids[:, None] * omegas[None, :]
    row_angle = row_ids[:, None] * omegas[None, :]
    return np.concatenate(
        [np.sin(col_angle), np.cos(col_angle), np.sin(row_angle), np.cos(row_angle)], axis=1
    ).astype(np.float32)

def cond_activation(step_ids, class_ids, class_table, w_freq, w_time):
    half_freq = FREQ // 2
    freqs = jnp.exp(-math.log(10000.0) * jnp.arange(half_freq, dtype=jnp.float32) / half_freq)
    tvalue = 1000.0 * (1.0 - step_ids.astype(jnp.float32) / STEPS)
    angles = tvalue[:, None] * freqs[None, :]
    embedded = jnp.concatenate([jnp.cos(angles), jnp.sin(angles)], axis=1).astype(jnp.bfloat16)
    hidden_time = jax.nn.silu(jnp.dot(embedded, w_freq, preferred_element_type=jnp.float32)).astype(
        jnp.bfloat16
    )
    condition = jnp.dot(hidden_time, w_time, preferred_element_type=jnp.float32) + jnp.take(
        class_table, class_ids, axis=0
    ).astype(jnp.float32)
    return jax.nn.silu(condition).astype(jnp.bfloat16)


def times_transposed(left, right):
    return lax.dot_general(
        left, right, (((1,), (1,)), ((), ())), preferred_element_type=jnp.float32
    )


def attention_product(rows_in, entry, head_count, head_size):
    qkv_width = 3 * head_count * head_size
    boundary = qkv_width // LANES * LANES
    rows = jnp.dot(rows_in, entry[:, :qkv_width], preferred_element_type=jnp.float32)
    rows = rows.astype(jnp.bfloat16)
    scale = 1.0 / math.sqrt(head_size)
    pieces = []
    if qkv_width > boundary:
        pieces.append(jnp.zeros((rows.shape[0], qkv_width - boundary), jnp.bfloat16))
    for head in range(head_count):
        start = head * 3 * head_size
        query = rows[:, start : start + head_size]
        keys = rows[:, start + head_size : start + 2 * head_size]
        values = rows[:, start + 2 * head_size : start + 3 * head_size]
        scores = times_transposed(query, keys)
        peak = jnp.max(scores, axis=-1, keepdims=True)
        weights = jnp.exp((scores - peak) * scale)
        total = jnp.sum(weights, axis=-1, keepdims=True)
        mixed = jnp.dot(
            weights.astype(jnp.bfloat16), values, preferred_element_type=jnp.float32
        )
        pieces.append((mixed / total).astype(jnp.bfloat16))
    attended = jnp.concatenate(pieces, axis=1)
    return times_transposed(attended, entry[:, boundary:])


class Gather:
    def __init__(self, sizes, own, buf, send_sem, z_sem, x_sem, y_sem, d_sem, p_sem):
        self.xs, self.ys, self.zs = sizes
        self.own, self.buf = own, buf
        self.send_sem, self.z_sem, self.x_sem = send_sem, z_sem, x_sem
        self.y_sem, self.d_sem, self.p_sem = y_sem, d_sem, p_sem
        tm, batch = lax.axis_index("tm"), lax.axis_index("batch")
        self.x, self.c = tm // CORES, tm % CORES
        self.z, self.y = batch // self.ys, batch % self.ys
        self.tm, self.batch = tm, batch
        rows = own.shape[1]
        self.cut = (rows // 32) * 16
        self.whole = pl.ds(0, rows)
        self.first = pl.ds(0, rows - self.cut)
        self.last = pl.ds(rows - self.cut, self.cut)

    def peer(self, position, step, size):
        return (position + step) % size

    def along_z(self, step):
        direction = 1 - 2 * (self.z * 2 // self.zs)
        return (self.z + direction * step + self.zs) % self.zs

    def device(self, x, c, z, y):
        return {"tm": x * CORES + c, "batch": z * self.ys + y}

    def peers(self):
        out = [self.device(self.x, 1 - self.c, self.z, self.y)]
        for step in range(1, self.zs):
            out.append(self.device(self.x, self.c, self.along_z(step), self.y))
        for step in range(1, self.xs):
            out.append(self.device(self.peer(self.x, step, self.xs), self.c, self.z, self.y))
        for step in range(1, self.ys):
            out.append(self.device(self.x, self.c, self.z, self.peer(self.y, step, self.ys)))
        return out

    def greet(self):
        barrier = pltpu.get_barrier_semaphore()
        for device in self.peers():
            pl.semaphore_signal(barrier, inc=1, device_id=device, device_id_type=MESH)

    def met(self):
        pl.semaphore_wait(pltpu.get_barrier_semaphore(), len(self.peers()))

    def place(self, k, x, z, y, rows):
        return self.buf.at[k, x * CORES + self.c, z * self.ys + y, rows]

    def send(self, k, kind, block, rows, device, arrival, own=False):
        target = self.place(k, *block, rows)
        source = self.own.at[k, rows] if own else target
        pltpu.make_async_remote_copy(
            src_ref=source,
            dst_ref=target,
            send_sem=self.send_sem.at[k, kind],
            recv_sem=arrival,
            device_id=device,
            device_id_type=MESH,
        ).start()

    def arrived(self, k, block, arrival):
        region = self.place(k, *block, self.whole)
        pltpu.make_async_copy(region, region, arrival).wait()

    def to_partner(self, k, block, own=False):
        device = self.device(self.x, 1 - self.c, self.z, self.y)
        self.send(k, 0, block, self.whole, device, self.p_sem.at[k, block[0]], own)

    def to_z(self, k):
        block = (self.x, self.z, self.y)
        for step in range(1, self.zs):
            device = self.device(self.x, self.c, self.along_z(step), self.y)
            self.send(k, 1, block, self.whole, device, self.z_sem.at[k, self.z], True)

    def to_x(self, k, block, own=False):
        for step in range(1, self.xs):
            device = self.device(self.peer(self.x, step, self.xs), self.c, self.z, self.y)
            arrival = self.x_sem.at[k, block[1] * self.xs + self.x]
            self.send(k, 2, block, self.whole, device, arrival, own)

    def to_y(self, k, block, own=False):
        for step in range(1, self.ys):
            device = self.device(self.x, self.c, self.z, self.peer(self.y, step, self.ys))
            arrival = self.y_sem.at[k, block[1] * self.ys + self.y]
            self.send(k, 3, block, self.whole, device, arrival, own)

    def own_out(self, k):
        block = (self.x, self.z, self.y)
        self.to_y(k, block, True)
        self.to_x(k, block, True)
        self.to_partner(k, block, True)

    def from_z(self, k, step):
        z = self.along_z(step)
        block = (self.x, z, self.y)
        self.arrived(k, block, self.z_sem.at[k, z])
        self.to_y(k, block)
        self.to_x(k, block)
        self.to_partner(k, block)

    def from_xy(self, k, step):
        z = self.along_z(step)
        for ystep in range(1, self.ys):
            y = self.peer(self.y, ystep, self.ys)
            block = (self.x, z, y)
            self.arrived(k, block, self.y_sem.at[k, z * self.ys + y])
            for step in range(1, self.xs):
                device = self.device(self.peer(self.x, step, self.xs), self.c, self.z, self.y)
                self.send(k, 4, block, self.first, device, self.d_sem.at[k, self.x])
            self.to_partner(k, block)
        for xstep in range(1, self.xs):
            x = self.peer(self.x, xstep, self.xs)
            block = (x, z, self.y)
            self.arrived(k, block, self.x_sem.at[k, z * self.xs + x])
            for step in range(1, self.ys):
                device = self.device(self.x, self.c, self.z, self.peer(self.y, step, self.ys))
                self.send(k, 4, block, self.last, device, self.d_sem.at[k, x])
            self.to_partner(k, block)

    def from_diagonal(self, k):
        count = self.zs * (self.ys - 1)
        for xstep in range(1, self.xs):
            x = self.peer(self.x, xstep, self.xs)
            if count:
                region = self.buf.at[k, 0, pl.ds(0, count)]
                pltpu.make_async_copy(region, region, self.d_sem.at[k, x]).wait()
            for ystep in range(1, self.ys):
                for z in range(self.zs):
                    self.to_partner(k, (x, z, self.peer(self.y, ystep, self.ys)))

    def from_partner(self, k, x):
        region = self.buf.at[k, 0]
        pltpu.make_async_copy(region, region, self.p_sem.at[k, x]).wait()

    def all_left(self, k):
        xs, ys, zs = self.xs, self.ys, self.zs
        regions = [self.buf.at[k, pl.ds(0, xs)]]
        regions.append(self.buf.at[k, 0, pl.ds(0, zs - 1)] if zs > 1 else None)
        regions.append(self.buf.at[k, pl.ds(0, xs - 1), pl.ds(0, zs)] if xs > 1 else None)
        regions.append(self.buf.at[k, 0, pl.ds(0, zs * (ys - 1))] if ys > 1 else None)
        both = xs > 1 and ys > 1
        regions.append(self.buf.at[k, pl.ds(0, xs - 1), pl.ds(0, zs * (ys - 1))] if both else None)
        for kind, region in enumerate(regions):
            if region is not None:
                pltpu.make_async_copy(region, region, self.send_sem.at[k, kind]).wait()


def denoise_kernel(
    sizes, head_count, head_size,
    patch_ref, mod_ref, w_patch_ref, w_final_ref, pos_ref, own_ref, out_ref,
    buf, tokens, normed, hidden, send_sem, z_sem, x_sem, y_sem, d_sem, p_sem,
):
    points, lane_rows, lanes = patch_ref.shape
    patch_size, width = w_patch_ref.shape
    group = lanes // patch_size
    token_count = lane_rows * group
    shards = sizes[0] * CORES
    block_rows, block_width = own_ref.shape[1:]
    gather = Gather(sizes, own_ref, buf, send_sem, z_sem, x_sem, y_sem, d_sem, p_sem)
    gather.greet()
    for k in range(3):
        buf[k, gather.tm, gather.batch] = own_ref[k]
    gather.met()
    gather.own_out(0)
    for k in range(3):
        gather.to_z(k)

    def part(point, index):
        return mod_ref[point, pl.ds(index, 1), :]

    def modulated(values, point, index):
        return (layer_norm(values) * (1.0 + part(point, index + 1)) + part(point, index)).astype(
            jnp.bfloat16
        )

    def enter(point, carry):
        flat = patch_ref[point]
        pieces = [flat[:, k * patch_size : (k + 1) * patch_size] for k in range(group)]
        value = jnp.dot(
            jnp.concatenate(pieces, axis=0), w_patch_ref[...], preferred_element_type=jnp.float32
        )
        value = value + pos_ref[...]
        tokens[point] = value
        normed[point] = modulated(value, point, 0)
        return carry

    lax.fori_loop(0, points, enter, 0)

    for step in range(sizes[2]):
        if step:
            gather.from_z(0, step)
        if step > 1:
            gather.from_xy(0, step - 2)
    gather.from_xy(0, max(sizes[2] - 2, 0))
    if sizes[2] > 1:
        gather.from_xy(0, sizes[2] - 1)
    gather.own_out(1)

    def weights(k, shard):
        return buf[k, shard].reshape(sizes[1] * sizes[2] * block_rows, block_width)

    def shard_of(turn):
        x = (gather.x + turn // CORES) % sizes[0]
        return x, x * CORES + (gather.c + turn % CORES) % CORES

    total_steps = shards * points

    def sweep(k, events, body):
        at = {}
        for share, event in events:
            at.setdefault(int(share * total_steps), []).append(event)

        def one(step, carry):
            turn, point = step // points, step % points
            x, shard = shard_of(turn)
            for when, todo in at.items():
                @pl.when(step == when)
                def _():
                    for event in todo:
                        event()

            @pl.when((point == 0) & (turn % CORES == 1))
            def _():
                gather.from_partner(k, x)

            body(shard, point)
            return carry

        lax.fori_loop(0, total_steps, one, 0)

    def relay(k, start, stop, last):
        todo = []
        zs = sizes[2]
        for step in range(1, zs):
            todo.append(functools.partial(gather.from_z, k, step))
            if step > 1:
                todo.append(functools.partial(gather.from_xy, k, step - 2))
        for step in range(max(zs - 2, 0), zs):
            todo.append(functools.partial(gather.from_xy, k, step))
        if last is not None:
            todo.append(functools.partial(gather.own_out, last))
        count = len(todo)
        return [(start + (stop - start) * i / max(count - 1, 1), e) for i, e in enumerate(todo)]

    def attention_step(shard, point):
        product = attention_product(normed[point], weights(0, shard), head_count, head_size)
        tokens[point] += part(point, 2) * product

    half = CORES / shards
    sweep(
        0,
        [(half, functools.partial(gather.from_diagonal, 0))] + relay(1, 0.1, 0.8, 2),
        attention_step,
    )

    def second(point, carry):
        normed[point] = modulated(tokens[point], point, 3)
        return carry

    lax.fori_loop(0, points, second, 0)

    def hidden_step(shard, point):
        value = jnp.dot(normed[point], weights(1, shard), preferred_element_type=jnp.float32)
        hidden[shard, point] = jax.nn.gelu(value, approximate=True).astype(jnp.bfloat16)

    sweep(
        1,
        [(half, functools.partial(gather.from_diagonal, 1))] + relay(2, 0.0, 0.95, None),
        hidden_step,
    )

    def residual_step(shard, point):
        product = times_transposed(hidden[shard, point], weights(2, shard))
        tokens[point] += part(point, 5) * product

    sweep(2, [(half, functools.partial(gather.from_diagonal, 2))], residual_step)

    def leave(point, carry):
        final_in = modulated(tokens[point], point, 6)
        value = jnp.dot(final_in, w_final_ref[...], preferred_element_type=jnp.float32)
        pieces = [value[k * lane_rows : (k + 1) * lane_rows, :] for k in range(group)]
        out_ref[point] = jnp.concatenate(pieces, axis=1).astype(jnp.bfloat16)
        return carry

    lax.fori_loop(0, points, leave, 0)
    for k in range(3):
        gather.all_left(k)


def denoise(patch_rows, modulation, w_patch, w_final, own, sizes):
    points, lane_rows, lanes = patch_rows.shape
    patch_size, width = w_patch.shape
    group = lanes // patch_size
    token_count = lane_rows * group
    xs, ys, zs = sizes
    shards, blocks = xs * CORES, ys * zs
    block_rows, block_width = own.shape[1:]
    pos = jnp.asarray(position_table(token_count, group))
    dma = pltpu.SemaphoreType.DMA
    head_size = width // HEADS
    vmem = pl.BlockSpec(memory_space=pltpu.VMEM)
    return pl.pallas_call(
        functools.partial(denoise_kernel, sizes, HEADS // shards, head_size),
        out_shape=jax.ShapeDtypeStruct(patch_rows.shape, jnp.bfloat16),
        in_specs=[vmem] * 6,
        out_specs=vmem,
        scratch_shapes=[
            pltpu.VMEM((3, shards, blocks, block_rows, block_width), jnp.bfloat16),
            pltpu.VMEM((points, token_count, width), jnp.float32),
            pltpu.VMEM((points, token_count, width), jnp.bfloat16),
            pltpu.VMEM((shards, points, token_count, block_width), jnp.bfloat16),
            dma((3, 5)),
            dma((3, zs)),
            dma((3, zs * xs)),
            dma((3, zs * ys)),
            dma((3, xs)),
            dma((3, xs)),
        ],
        compiler_params=pltpu.CompilerParams(
            collective_id=0, has_side_effects=True, vmem_limit_bytes=66_000_000
        ),
        name="denoise",
    )(patch_rows, modulation, w_patch, w_final, pos, own)


def add_pair(earlier, later):
    return earlier + later


def local(
    sizes,
    latents,
    shifts,
    starts,
    labels,
    class_table,
    w_freq,
    w_time,
    w_ada,
    w_patch,
    w_qkv,
    w_proj,
    w_fc1,
    w_fc2,
    w_final,
):
    tm_count = lax.axis_size("tm")
    tm_index = lax.axis_index("tm")
    batch_index = lax.axis_index("batch")
    local_steps = latents.shape[0]
    window = local_steps * tm_count
    sample_total, lat_block = latents.shape[1:]
    lane_rows = lat_block // LANES
    whole = lax.all_gather(latents, "tm", axis=0, tiled=True)
    local_positions = tm_index * local_steps + jnp.arange(local_steps, dtype=jnp.int32)[:, None]
    source_rows = jnp.minimum(local_positions + shifts[None, :], window - 1)
    points = jnp.take_along_axis(whole, source_rows[:, :, None], axis=0)
    anchor = jnp.take_along_axis(whole, shifts[None, :, None], axis=0)[0]
    by_sample = lax.all_to_all(
        points.astype(jnp.bfloat16).reshape(local_steps, sample_total, lane_rows, LANES),
        "batch",
        split_axis=1,
        concat_axis=2,
        tiled=True,
    )
    sample_count = by_sample.shape[1]
    own_shifts = lax.dynamic_slice_in_dim(shifts, batch_index * sample_count, sample_count)
    own_starts = lax.dynamic_slice_in_dim(starts, batch_index * sample_count, sample_count)
    own_labels = lax.dynamic_slice_in_dim(labels, batch_index * sample_count, sample_count)
    window_positions = jnp.arange(window, dtype=jnp.int32)[:, None]
    step_ids = (own_starts + own_shifts)[None, :] + window_positions
    class_ids = jnp.broadcast_to(own_labels[None, :], step_ids.shape)
    activation = cond_activation(
        step_ids.reshape(-1), class_ids.reshape(-1), class_table, w_freq, w_time
    )
    own_columns = jnp.dot(activation, w_ada, preferred_element_type=jnp.float32).astype(
        jnp.bfloat16
    )
    modulation = lax.all_to_all(own_columns, "tm", split_axis=0, concat_axis=1, tiled=True)
    point_count = local_steps * sample_count
    point_rows = by_sample.reshape(point_count, -1, LANES)
    own = jnp.stack([jnp.concatenate([w_qkv, w_proj.T], axis=1), w_fc1, w_fc2.T])
    parts = modulation.astype(jnp.float32).reshape(point_count, 8, -1)
    velocity_mid = denoise(point_rows, parts, w_patch, w_final, own, sizes)
    velocity_mid = velocity_mid.reshape(local_steps, sample_count, -1, LANES)
    velocity_out = lax.all_to_all(velocity_mid, "batch", split_axis=2, concat_axis=1, tiled=True)
    velocity_out = velocity_out.reshape(local_steps, sample_total, lat_block)
    velocity_float = velocity_out.astype(jnp.float32)
    summed = jnp.cumsum(velocity_float, axis=0)
    running = jnp.concatenate([jnp.zeros_like(summed[:1]), summed[:-1]], axis=0)
    block_sum = jnp.sum(velocity_float, axis=0)
    earlier_sum = entering(block_sum, "tm", add_pair, jnp.zeros_like(block_sum))
    latents_out = anchor[None] + (earlier_sum[None] + running) * (1.0 / STEPS)
    return (latents_out, velocity_out)


def chip_sizes(mesh):
    batch = mesh.shape["batch"]
    ys = 1
    while ys * ys * 4 <= batch:
        ys *= 2
    return mesh.shape["tm"] // CORES, ys, batch // ys


def solution(mesh):
    placed = (
        P("tm", None, "batch"),
        P(),
        P(),
        P(),
        P(),
        P(),
        P(),
        P(None, "tm"),
        P(),
        P("batch", "tm"),
        P("tm", "batch"),
        P("batch", "tm"),
        P("tm", "batch"),
        P(),
    )
    return jax.shard_map(
        functools.partial(local, chip_sizes(mesh)),
        mesh=mesh,
        in_specs=placed,
        out_specs=(P("tm", None, "batch"), P("tm", None, "batch")),
        check_vma=False,
    )
```

```python
import functools
import math

import jax
import jax.numpy as jnp
import numpy as np
from jax import lax
from jax.experimental import pallas as pl
from jax.experimental.pallas import tpu as pltpu
from jax.sharding import PartitionSpec as P

D = 1152
HEADS = 16
FREQ = 256
GRID = 16
STEPS = 18
LANES = 128
CORES = 2
MESH = pl.DeviceIdType.MESH


def layer_norm(values):
    average = jnp.mean(values, axis=-1, keepdims=True)
    centred = values - average
    variance = jnp.mean(centred * centred, axis=-1, keepdims=True)
    return centred * lax.rsqrt(variance + 1e-06)


def position_table(token_count, group):
    token_ids = np.arange(token_count).reshape(token_count // group, group).T.reshape(-1)
    row_ids = (token_ids // GRID).astype(np.float32)
    col_ids = (token_ids % GRID).astype(np.float32)
    quarter = D // 4
    omegas = np.exp(-math.log(10000.0) * np.arange(quarter, dtype=np.float32) / quarter).astype(np.float32)
    col_angle = col_ids[:, None] * omegas[None, :]
    row_angle = row_ids[:, None] * omegas[None, :]
    return np.concatenate(
        [np.sin(col_angle), np.cos(col_angle), np.sin(row_angle), np.cos(row_angle)], axis=1
    ).astype(np.float32)

def cond_activation(step_ids, class_ids, class_table, w_freq, w_time):
    half_freq = FREQ // 2
    freqs = jnp.exp(-math.log(10000.0) * jnp.arange(half_freq, dtype=jnp.float32) / half_freq)
    tvalue = 1000.0 * (1.0 - step_ids.astype(jnp.float32) / STEPS)
    angles = tvalue[:, None] * freqs[None, :]
    embedded = jnp.concatenate([jnp.cos(angles), jnp.sin(angles)], axis=1).astype(jnp.bfloat16)
    hidden_time = jax.nn.silu(jnp.dot(embedded, w_freq, preferred_element_type=jnp.float32)).astype(
        jnp.bfloat16
    )
    condition = jnp.dot(hidden_time, w_time, preferred_element_type=jnp.float32) + jnp.take(
        class_table, class_ids, axis=0
    ).astype(jnp.float32)
    return jax.nn.silu(condition).astype(jnp.bfloat16)


def times_transposed(left, right):
    return lax.dot_general(
        left, right, (((1,), (1,)), ((), ())), preferred_element_type=jnp.float32
    )


def attention_product(rows_in, entry, head_count, head_size):
    qkv_width = 3 * head_count * head_size
    boundary = qkv_width // LANES * LANES
    rows = jnp.dot(rows_in, entry[:, :qkv_width], preferred_element_type=jnp.float32)
    rows = rows.astype(jnp.bfloat16)
    scale = 1.0 / math.sqrt(head_size)
    pieces = []
    if qkv_width > boundary:
        pieces.append(jnp.zeros((rows.shape[0], qkv_width - boundary), jnp.bfloat16))
    for head in range(head_count):
        start = head * 3 * head_size
        query = rows[:, start : start + head_size]
        keys = rows[:, start + head_size : start + 2 * head_size]
        values = rows[:, start + 2 * head_size : start + 3 * head_size]
        scores = times_transposed(query, keys)
        peak = jnp.max(scores, axis=-1, keepdims=True)
        weights = jnp.exp((scores - peak) * scale)
        total = jnp.sum(weights, axis=-1, keepdims=True)
        mixed = jnp.dot(
            weights.astype(jnp.bfloat16), values, preferred_element_type=jnp.float32
        )
        pieces.append((mixed / total).astype(jnp.bfloat16))
    attended = jnp.concatenate(pieces, axis=1)
    return times_transposed(attended, entry[:, boundary:])


class Gather:
    def __init__(self, sizes, own, buf, send_sem, z_sem, x_sem, y_sem, d_sem, p_sem):
        self.xs, self.ys, self.zs = sizes
        self.own, self.buf = own, buf
        self.send_sem, self.z_sem, self.x_sem = send_sem, z_sem, x_sem
        self.y_sem, self.d_sem, self.p_sem = y_sem, d_sem, p_sem
        tm, batch = lax.axis_index("tm"), lax.axis_index("batch")
        self.x, self.c = tm // CORES, tm % CORES
        self.z, self.y = batch // self.ys, batch % self.ys
        self.tm, self.batch = tm, batch
        rows = own.shape[1]
        self.cut = (rows // 32) * 16
        self.whole = pl.ds(0, rows)
        self.first = pl.ds(0, rows - self.cut)
        self.last = pl.ds(rows - self.cut, self.cut)

    def peer(self, position, step, size):
        return (position + step) % size

    def along_z(self, step):
        direction = 1 - 2 * (self.z * 2 // self.zs)
        return (self.z + direction * step + self.zs) % self.zs

    def device(self, x, c, z, y):
        return {"tm": x * CORES + c, "batch": z * self.ys + y}

    def tm_peers(self):
        count = self.xs * CORES
        return [{"tm": (self.tm + i) % count, "batch": self.batch} for i in range(1, count)]

    def batch_peers(self):
        count = self.ys * self.zs
        return [{"tm": self.tm, "batch": (self.batch + i) % count} for i in range(1, count)]

    def peers(self):
        return self.tm_peers() + self.batch_peers()

    def greet(self):
        barrier = pltpu.get_barrier_semaphore()
        for device in self.peers():
            pl.semaphore_signal(barrier, inc=1, device_id=device, device_id_type=MESH)

    def met(self):
        pl.semaphore_wait(pltpu.get_barrier_semaphore(), len(self.peers()))

    def place(self, k, x, z, y, rows):
        return self.buf.at[k, x * CORES + self.c, z * self.ys + y, rows]

    def send(self, k, kind, block, rows, device, arrival, own=False):
        target = self.place(k, *block, rows)
        source = self.own.at[k, rows] if own else target
        pltpu.make_async_remote_copy(
            src_ref=source,
            dst_ref=target,
            send_sem=self.send_sem.at[k, kind],
            recv_sem=arrival,
            device_id=device,
            device_id_type=MESH,
        ).start()

    def arrived(self, k, block, arrival):
        region = self.place(k, *block, self.whole)
        pltpu.make_async_copy(region, region, arrival).wait()

    def to_partner(self, k, block, own=False):
        device = self.device(self.x, 1 - self.c, self.z, self.y)
        self.send(k, 0, block, self.whole, device, self.p_sem.at[k, block[0]], own)

    def to_z(self, k):
        block = (self.x, self.z, self.y)
        for step in range(1, self.zs):
            device = self.device(self.x, self.c, self.along_z(step), self.y)
            self.send(k, 1, block, self.whole, device, self.z_sem.at[k, self.z], True)

    def to_x(self, k, block, own=False):
        for step in range(1, self.xs):
            device = self.device(self.peer(self.x, step, self.xs), self.c, self.z, self.y)
            arrival = self.x_sem.at[k, block[1] * self.xs + self.x]
            self.send(k, 2, block, self.whole, device, arrival, own)

    def to_y(self, k, block, own=False):
        for step in range(1, self.ys):
            device = self.device(self.x, self.c, self.z, self.peer(self.y, step, self.ys))
            arrival = self.y_sem.at[k, block[1] * self.ys + self.y]
            self.send(k, 3, block, self.whole, device, arrival, own)

    def own_out(self, k):
        block = (self.x, self.z, self.y)
        self.to_y(k, block, True)
        self.to_x(k, block, True)
        self.to_partner(k, block, True)

    def from_z(self, k, step):
        z = self.along_z(step)
        block = (self.x, z, self.y)
        self.arrived(k, block, self.z_sem.at[k, z])
        self.to_y(k, block)
        self.to_x(k, block)
        self.to_partner(k, block)

    def from_xy(self, k, step):
        z = self.along_z(step)
        for ystep in range(1, self.ys):
            y = self.peer(self.y, ystep, self.ys)
            block = (self.x, z, y)
            self.arrived(k, block, self.y_sem.at[k, z * self.ys + y])
            for step in range(1, self.xs):
                device = self.device(self.peer(self.x, step, self.xs), self.c, self.z, self.y)
                self.send(k, 4, block, self.first, device, self.d_sem.at[k, self.x])
            self.to_partner(k, block)
        for xstep in range(1, self.xs):
            x = self.peer(self.x, xstep, self.xs)
            block = (x, z, self.y)
            self.arrived(k, block, self.x_sem.at[k, z * self.xs + x])
            for step in range(1, self.ys):
                device = self.device(self.x, self.c, self.z, self.peer(self.y, step, self.ys))
                self.send(k, 4, block, self.last, device, self.d_sem.at[k, x])
            self.to_partner(k, block)

    def from_diagonal(self, k):
        count = self.zs * (self.ys - 1)
        for xstep in range(1, self.xs):
            x = self.peer(self.x, xstep, self.xs)
            if count:
                region = self.buf.at[k, 0, pl.ds(0, count)]
                pltpu.make_async_copy(region, region, self.d_sem.at[k, x]).wait()
            for ystep in range(1, self.ys):
                for z in range(self.zs):
                    self.to_partner(k, (x, z, self.peer(self.y, ystep, self.ys)))

    def from_partner(self, k, x):
        region = self.buf.at[k, 0]
        pltpu.make_async_copy(region, region, self.p_sem.at[k, x]).wait()

    def all_left(self, k):
        xs, ys, zs = self.xs, self.ys, self.zs
        regions = [self.buf.at[k, pl.ds(0, xs)]]
        regions.append(self.buf.at[k, 0, pl.ds(0, zs - 1)] if zs > 1 else None)
        regions.append(self.buf.at[k, pl.ds(0, xs - 1), pl.ds(0, zs)] if xs > 1 else None)
        regions.append(self.buf.at[k, 0, pl.ds(0, zs * (ys - 1))] if ys > 1 else None)
        both = xs > 1 and ys > 1
        regions.append(self.buf.at[k, pl.ds(0, xs - 1), pl.ds(0, zs * (ys - 1))] if both else None)
        for kind, region in enumerate(regions):
            if region is not None:
                pltpu.make_async_copy(region, region, self.send_sem.at[k, kind]).wait()


class Exchange:
    def __init__(self, index, sent, landed, send_sem, recv_sem, peers, axis):
        self.sent, self.landed, self.peers, self.axis = sent, landed, peers, axis
        self.send_sem, self.recv_sem = send_sem.at[index], recv_sem.at[index]

    def start(self, me, source=None):
        for peer in self.peers:
            block = self.sent.at[peer[self.axis]] if source is None else source
            pltpu.make_async_remote_copy(
                src_ref=block,
                dst_ref=self.landed.at[me],
                send_sem=self.send_sem,
                recv_sem=self.recv_sem,
                device_id=peer,
                device_id_type=MESH,
            ).start()

    def region(self):
        return self.landed.at[pl.ds(0, len(self.peers))]

    def arrived(self):
        pltpu.make_async_copy(self.region(), self.region(), self.recv_sem).wait()

    def left(self):
        pltpu.make_async_copy(self.region(), self.region(), self.send_sem).wait()


def denoise_kernel(
    sizes, head_count, head_size,
    shift_ref, latent_ref, act_ref, w_patch_ref, w_final_ref, pos_ref, own_ref, w_ada_hbm,
    latent_out, velocity_out,
    buf, tokens, normed, hidden, w_ada, window, sent_points, landed_points, sent_mod, landed_mod,
    sent_velocity, landed_velocity, sent_sums, landed_sums, anchors, rows_in,
    send_sem, z_sem, x_sem, y_sem, d_sem, p_sem, ex_send, ex_recv, ada_sem,
):
    steps, samples, lane_rows, lanes = latent_ref.shape
    patch_size, width = w_patch_ref.shape
    group = lanes // patch_size
    shards, blocks = sizes[0] * CORES, sizes[1] * sizes[2]
    own_samples = samples // blocks
    points = steps * own_samples
    block_rows, block_width = own_ref.shape[1:]
    columns = w_ada_hbm.shape[1]
    fetch_ada = pltpu.make_async_copy(w_ada_hbm, w_ada, ada_sem)
    fetch_ada.start()
    gather = Gather(sizes, own_ref, buf, send_sem, z_sem, x_sem, y_sem, d_sem, p_sem)
    tm, batch = gather.tm, gather.batch
    tm_peers, batch_peers = gather.tm_peers(), gather.batch_peers()
    ex = functools.partial(Exchange, send_sem=ex_send, recv_sem=ex_recv)
    latent_ex = ex(0, None, window, peers=tm_peers, axis="tm")
    mod_ex = ex(1, sent_mod, landed_mod, peers=tm_peers, axis="tm")
    point_ex = ex(2, sent_points, landed_points, peers=batch_peers, axis="batch")
    velocity_ex = ex(3, sent_velocity, landed_velocity, peers=batch_peers, axis="batch")
    sum_ex = ex(4, None, landed_sums, peers=tm_peers, axis="tm")
    gather.greet()
    window[tm] = latent_ref[...]
    for k in range(3):
        buf[k, tm, batch] = own_ref[k]
    gather.met()
    latent_ex.start(tm, latent_ref)
    gather.own_out(0)
    for k in range(3):
        gather.to_z(k)

    fetch_ada.wait()
    mod = jnp.dot(act_ref[...], w_ada[...], preferred_element_type=jnp.float32)
    mod = mod.astype(jnp.bfloat16).astype(jnp.float32)
    for i in range(shards):
        sent_mod[i] = mod[i * points : (i + 1) * points]
    landed_mod[tm] = sent_mod[tm]
    latent_ex.arrived()
    mod_ex.start(tm)
    for sample in range(samples):
        shift = shift_ref[sample]
        anchors[sample] = window[shift // steps, shift % steps, sample]
        for step in range(steps):
            source = jnp.minimum(tm * steps + step + shift, shards * steps - 1)
            place = step * own_samples + sample % own_samples
            sent_points[sample // own_samples, place] = window[
                source // steps, source % steps, sample
            ]
    landed_points[batch] = sent_points[batch]
    point_ex.start(batch)
    gather.from_z(0, 1)
    mod_ex.arrived()
    point_ex.arrived()

    def part(point, index):
        pieces, at = [], index * width
        while at < (index + 1) * width:
            start = at % columns
            size = min(columns - start, (index + 1) * width - at)
            pieces.append(landed_mod[at // columns, pl.ds(point, 1), start : start + size])
            at += size
        return pieces[0] if len(pieces) == 1 else jnp.concatenate(pieces, axis=1)

    def modulated(values, point, index):
        return (layer_norm(values) * (1.0 + part(point, index + 1)) + part(point, index)).astype(
            jnp.bfloat16
        )

    def enter(point, carry):
        for block in range(blocks):
            rows_in[block * lane_rows : (block + 1) * lane_rows, :] = landed_points[block, point]
        flat = rows_in[...].astype(jnp.bfloat16)
        pieces = [flat[:, k * patch_size : (k + 1) * patch_size] for k in range(group)]
        value = jnp.dot(
            jnp.concatenate(pieces, axis=0), w_patch_ref[...], preferred_element_type=jnp.float32
        )
        value = value + pos_ref[...]
        tokens[point] = value
        normed[point] = modulated(value, point, 0)
        return carry

    lax.fori_loop(0, points, enter, 0)

    for step in range(sizes[2]):
        if step > 1:
            gather.from_z(0, step)
        if step > 1:
            gather.from_xy(0, step - 2)
    gather.from_xy(0, max(sizes[2] - 2, 0))
    if sizes[2] > 1:
        gather.from_xy(0, sizes[2] - 1)
    gather.own_out(1)

    def weights(k, shard):
        return buf[k, shard].reshape(sizes[1] * sizes[2] * block_rows, block_width)

    def shard_of(turn):
        x = (gather.x + turn // CORES) % sizes[0]
        return x, x * CORES + (gather.c + turn % CORES) % CORES

    total_steps = shards * points

    def sweep(k, events, body):
        at = {}
        for share, event in events:
            at.setdefault(int(share * total_steps), []).append(event)

        def one(step, carry):
            turn, point = step // points, step % points
            x, shard = shard_of(turn)
            for when, todo in at.items():
                @pl.when(step == when)
                def _():
                    for event in todo:
                        event()

            @pl.when((point == 0) & (turn % CORES == 1))
            def _():
                gather.from_partner(k, x)

            body(shard, point)
            return carry

        lax.fori_loop(0, total_steps, one, 0)

    def relay(k, start, stop, last):
        todo = []
        zs = sizes[2]
        for step in range(1, zs):
            todo.append(functools.partial(gather.from_z, k, step))
            if step > 1:
                todo.append(functools.partial(gather.from_xy, k, step - 2))
        for step in range(max(zs - 2, 0), zs):
            todo.append(functools.partial(gather.from_xy, k, step))
        if last is not None:
            todo.append(functools.partial(gather.own_out, last))
        count = len(todo)
        return [(start + (stop - start) * i / max(count - 1, 1), e) for i, e in enumerate(todo)]

    def attention_step(shard, point):
        product = attention_product(normed[point], weights(0, shard), head_count, head_size)
        tokens[point] += part(point, 2) * product

    half = CORES / shards
    sweep(
        0,
        [(half, functools.partial(gather.from_diagonal, 0))] + relay(1, 0.1, 0.8, 2),
        attention_step,
    )

    def second(point, carry):
        normed[point] = modulated(tokens[point], point, 3)
        return carry

    lax.fori_loop(0, points, second, 0)

    def hidden_step(shard, point):
        value = jnp.dot(normed[point], weights(1, shard), preferred_element_type=jnp.float32)
        hidden[shard, point] = jax.nn.gelu(value, approximate=True).astype(jnp.bfloat16)

    sweep(
        1,
        [(half, functools.partial(gather.from_diagonal, 1))] + relay(2, 0.0, 0.95, None),
        hidden_step,
    )

    def residual_step(shard, point):
        product = times_transposed(hidden[shard, point], weights(2, shard))
        tokens[point] += part(point, 5) * product

    sweep(2, [(half, functools.partial(gather.from_diagonal, 2))], residual_step)

    def leave(point, carry):
        final_in = modulated(tokens[point], point, 6)
        value = jnp.dot(final_in, w_final_ref[...], preferred_element_type=jnp.float32)
        flat_rows = blocks * lane_rows
        pieces = [value[k * flat_rows : (k + 1) * flat_rows, :] for k in range(group)]
        flat = jnp.concatenate(pieces, axis=1).astype(jnp.bfloat16).astype(jnp.float32)
        for block in range(blocks):
            sent_velocity[block, point] = flat[block * lane_rows : (block + 1) * lane_rows]
        return carry

    lax.fori_loop(0, points, leave, 0)
    landed_velocity[batch] = sent_velocity[batch]
    velocity_ex.start(batch)
    velocity_ex.arrived()

    def step_velocity(step):
        value = landed_velocity[:, step * own_samples : (step + 1) * own_samples]
        return value.reshape(samples, lane_rows, lanes)

    total = step_velocity(0)
    for step in range(1, steps):
        total = total + step_velocity(step)
    sent_sums[...] = total
    sum_ex.start(tm, sent_sums)
    for step in range(steps):
        velocity_out[step] = step_velocity(step)
    sum_ex.arrived()
    running = jnp.zeros_like(total)
    for i in range(shards):
        running = running + jnp.where(i < tm, landed_sums[i], 0.0)
    for step in range(steps):
        latent_out[step] = anchors[...] + running * (1.0 / STEPS)
        running = running + step_velocity(step)
    for exchange in (latent_ex, mod_ex, point_ex, velocity_ex, sum_ex):
        exchange.left()
    for k in range(3):
        gather.all_left(k)


def denoise(shifts, latents, activation, w_ada, w_patch, w_final, own, sizes):
    steps, samples, lane_rows, lanes = latents.shape
    patch_size, width = w_patch.shape
    group = lanes // patch_size
    xs, ys, zs = sizes
    shards, blocks = xs * CORES, ys * zs
    token_count = blocks * lane_rows * group
    points = steps * samples // blocks
    block_rows, block_width = own.shape[1:]
    pos = jnp.asarray(position_table(token_count, group))
    dma = pltpu.SemaphoreType.DMA
    head_size = width // HEADS
    vmem = pl.BlockSpec(memory_space=pltpu.VMEM)
    smem = pl.BlockSpec(memory_space=pltpu.SMEM)
    result = jax.ShapeDtypeStruct(latents.shape, jnp.float32)
    pieces = pltpu.VMEM((blocks, points, lane_rows, lanes), jnp.float32)
    sums = (samples, lane_rows, lanes)
    mod = pltpu.VMEM((shards, points, w_ada.shape[1]), jnp.float32)
    return pl.pallas_call(
        functools.partial(denoise_kernel, sizes, HEADS // shards, head_size),
        out_shape=(result, result),
        in_specs=[smem] + [vmem] * 6 + [pl.BlockSpec(memory_space=pl.ANY)],
        out_specs=(vmem, vmem),
        scratch_shapes=[
            pltpu.VMEM((3, shards, blocks, block_rows, block_width), jnp.bfloat16),
            pltpu.VMEM((points, token_count, width), jnp.float32),
            pltpu.VMEM((points, token_count, width), jnp.bfloat16),
            pltpu.VMEM((shards, points, token_count, block_width), jnp.bfloat16),
            pltpu.VMEM(w_ada.shape, jnp.bfloat16),
            pltpu.VMEM((shards, *latents.shape), jnp.float32),
            pieces,
            pieces,
            mod,
            mod,
            pieces,
            pieces,
            pltpu.VMEM(sums, jnp.float32),
            pltpu.VMEM((shards, *sums), jnp.float32),
            pltpu.VMEM(sums, jnp.float32),
            pltpu.VMEM((blocks * lane_rows, lanes), jnp.float32),
            dma((3, 5)),
            dma((3, zs)),
            dma((3, zs * xs)),
            dma((3, zs * ys)),
            dma((3, xs)),
            dma((3, xs)),
            dma((5,)),
            dma((5,)),
            dma,
        ],
        compiler_params=pltpu.CompilerParams(
            collective_id=0, has_side_effects=True, vmem_limit_bytes=67_000_000
        ),
        name="denoise",
    )(shifts, latents, activation, w_patch, w_final, pos, own, w_ada)


def local(
    sizes,
    latents,
    shifts,
    starts,
    labels,
    class_table,
    w_freq,
    w_time,
    w_ada,
    w_patch,
    w_qkv,
    w_proj,
    w_fc1,
    w_fc2,
    w_final,
):
    batch_index = lax.axis_index("batch")
    local_steps, sample_total, lat_block = latents.shape
    window = local_steps * lax.axis_size("tm")
    sample_count = sample_total // lax.axis_size("batch")
    own_shifts = lax.dynamic_slice_in_dim(shifts, batch_index * sample_count, sample_count)
    own_starts = lax.dynamic_slice_in_dim(starts, batch_index * sample_count, sample_count)
    own_labels = lax.dynamic_slice_in_dim(labels, batch_index * sample_count, sample_count)
    window_positions = jnp.arange(window, dtype=jnp.int32)[:, None]
    step_ids = (own_starts + own_shifts)[None, :] + window_positions
    class_ids = jnp.broadcast_to(own_labels[None, :], step_ids.shape)
    activation = cond_activation(
        step_ids.reshape(-1), class_ids.reshape(-1), class_table, w_freq, w_time
    )
    own = jnp.stack([jnp.concatenate([w_qkv, w_proj.T], axis=1), w_fc1, w_fc2.T])
    rows = latents.reshape(local_steps, sample_total, lat_block // LANES, LANES)
    latents_out, velocity = denoise(shifts, rows, activation, w_ada, w_patch, w_final, own, sizes)
    return (
        latents_out.reshape(latents.shape),
        velocity.astype(jnp.bfloat16).reshape(latents.shape),
    )


def chip_sizes(mesh):
    batch = mesh.shape["batch"]
    ys = 1
    while ys * ys * 4 <= batch:
        ys *= 2
    return mesh.shape["tm"] // CORES, ys, batch // ys


def solution(mesh):
    placed = (
        P("tm", None, "batch"),
        P(),
        P(),
        P(),
        P(),
        P(),
        P(),
        P(None, "tm"),
        P(),
        P("batch", "tm"),
        P("tm", "batch"),
        P("batch", "tm"),
        P("tm", "batch"),
        P(),
    )
    return jax.shard_map(
        functools.partial(local, chip_sizes(mesh)),
        mesh=mesh,
        in_specs=placed,
        out_specs=(P("tm", None, "batch"), P("tm", None, "batch")),
        check_vma=False,
    )
```

```python
import functools
import math

import jax
import jax.numpy as jnp
import numpy as np
from jax import lax
from jax.experimental import pallas as pl
from jax.experimental.pallas import tpu as pltpu
from jax.sharding import PartitionSpec as P

D = 1152
HEADS = 16
FREQ = 256
GRID = 16
STEPS = 18
LANES = 128
CORES = 2
MESH = pl.DeviceIdType.MESH


def layer_norm(values):
    average = jnp.mean(values, axis=-1, keepdims=True)
    centred = values - average
    variance = jnp.mean(centred * centred, axis=-1, keepdims=True)
    return centred * lax.rsqrt(variance + 1e-06)


def position_table(token_count, group):
    token_ids = np.arange(token_count).reshape(token_count // group, group).T.reshape(-1)
    row_ids = (token_ids // GRID).astype(np.float32)
    col_ids = (token_ids % GRID).astype(np.float32)
    quarter = D // 4
    omegas = np.exp(-math.log(10000.0) * np.arange(quarter, dtype=np.float32) / quarter).astype(np.float32)
    col_angle = col_ids[:, None] * omegas[None, :]
    row_angle = row_ids[:, None] * omegas[None, :]
    return np.concatenate(
        [np.sin(col_angle), np.cos(col_angle), np.sin(row_angle), np.cos(row_angle)], axis=1
    ).astype(np.float32)

def step_table(count):
    half_freq = FREQ // 2
    freqs = np.exp(-math.log(10000.0) * np.arange(half_freq, dtype=np.float32) / half_freq)
    tvalue = 1000.0 * (1.0 - np.arange(count, dtype=np.float32) / np.float32(STEPS))
    angles = tvalue.astype(np.float32)[:, None] * freqs.astype(np.float32)[None, :]
    return np.concatenate([np.cos(angles), np.sin(angles)], axis=1).astype(np.float32)


def times_transposed(left, right):
    return lax.dot_general(
        left, right, (((1,), (1,)), ((), ())), preferred_element_type=jnp.float32
    )


def attention_product(rows_in, entry, head_count, head_size):
    qkv_width = 3 * head_count * head_size
    boundary = qkv_width // LANES * LANES
    rows = jnp.dot(rows_in, entry[:, :qkv_width], preferred_element_type=jnp.float32)
    rows = rows.astype(jnp.bfloat16)
    scale = 1.0 / math.sqrt(head_size)
    pieces = []
    if qkv_width > boundary:
        pieces.append(jnp.zeros((rows.shape[0], qkv_width - boundary), jnp.bfloat16))
    for head in range(head_count):
        start = head * 3 * head_size
        query = rows[:, start : start + head_size]
        keys = rows[:, start + head_size : start + 2 * head_size]
        values = rows[:, start + 2 * head_size : start + 3 * head_size]
        scores = times_transposed(query, keys)
        peak = jnp.max(scores, axis=-1, keepdims=True)
        weights = jnp.exp((scores - peak) * scale)
        total = jnp.sum(weights, axis=-1, keepdims=True)
        mixed = jnp.dot(
            weights.astype(jnp.bfloat16), values, preferred_element_type=jnp.float32
        )
        pieces.append((mixed / total).astype(jnp.bfloat16))
    attended = jnp.concatenate(pieces, axis=1)
    return times_transposed(attended, entry[:, boundary:])


class Gather:
    def __init__(self, sizes, own, buf, send_sem, z_sem, x_sem, y_sem, d_sem, p_sem):
        self.xs, self.ys, self.zs = sizes
        self.own, self.buf = own, buf
        self.send_sem, self.z_sem, self.x_sem = send_sem, z_sem, x_sem
        self.y_sem, self.d_sem, self.p_sem = y_sem, d_sem, p_sem
        tm, batch = lax.axis_index("tm"), lax.axis_index("batch")
        self.x, self.c = tm // CORES, tm % CORES
        self.z, self.y = batch // self.ys, batch % self.ys
        self.tm, self.batch = tm, batch
        rows = own.shape[1]
        self.cut = (rows // 32) * 16
        self.whole = pl.ds(0, rows)
        self.first = pl.ds(0, rows - self.cut)
        self.last = pl.ds(rows - self.cut, self.cut)

    def peer(self, position, step, size):
        return (position + step) % size

    def along_z(self, step):
        direction = 1 - 2 * (self.z * 2 // self.zs)
        return (self.z + direction * step + self.zs) % self.zs

    def device(self, x, c, z, y):
        return {"tm": x * CORES + c, "batch": z * self.ys + y}

    def tm_peers(self):
        count = self.xs * CORES
        return [{"tm": (self.tm + i) % count, "batch": self.batch} for i in range(1, count)]

    def batch_peers(self):
        count = self.ys * self.zs
        return [{"tm": self.tm, "batch": (self.batch + i) % count} for i in range(1, count)]

    def peers(self):
        return self.tm_peers() + self.batch_peers()

    def greet(self):
        barrier = pltpu.get_barrier_semaphore()
        for device in self.peers():
            pl.semaphore_signal(barrier, inc=1, device_id=device, device_id_type=MESH)

    def met(self):
        pl.semaphore_wait(pltpu.get_barrier_semaphore(), len(self.peers()))

    def place(self, k, x, z, y, rows):
        return self.buf.at[k, x * CORES + self.c, z * self.ys + y, rows]

    def send(self, k, kind, block, rows, device, arrival, own=False):
        target = self.place(k, *block, rows)
        source = self.own.at[k, rows] if own else target
        pltpu.make_async_remote_copy(
            src_ref=source,
            dst_ref=target,
            send_sem=self.send_sem.at[k, kind],
            recv_sem=arrival,
            device_id=device,
            device_id_type=MESH,
        ).start()

    def arrived(self, k, block, arrival):
        region = self.place(k, *block, self.whole)
        pltpu.make_async_copy(region, region, arrival).wait()

    def to_partner(self, k, block, own=False):
        device = self.device(self.x, 1 - self.c, self.z, self.y)
        self.send(k, 0, block, self.whole, device, self.p_sem.at[k, block[0]], own)

    def to_z(self, k, steps):
        block = (self.x, self.z, self.y)
        for step in steps:
            device = self.device(self.x, self.c, self.along_z(step), self.y)
            self.send(k, 1, block, self.whole, device, self.z_sem.at[k, self.z], True)

    def to_x(self, k, block, own=False):
        for step in range(1, self.xs):
            device = self.device(self.peer(self.x, step, self.xs), self.c, self.z, self.y)
            arrival = self.x_sem.at[k, block[1] * self.xs + self.x]
            self.send(k, 2, block, self.whole, device, arrival, own)

    def to_y(self, k, block, own=False):
        for step in range(1, self.ys):
            device = self.device(self.x, self.c, self.z, self.peer(self.y, step, self.ys))
            arrival = self.y_sem.at[k, block[1] * self.ys + self.y]
            self.send(k, 3, block, self.whole, device, arrival, own)

    def own_out(self, k):
        block = (self.x, self.z, self.y)
        self.to_y(k, block, True)
        self.to_x(k, block, True)
        self.to_partner(k, block, True)

    def from_z(self, k, step):
        z = self.along_z(step)
        block = (self.x, z, self.y)
        self.arrived(k, block, self.z_sem.at[k, z])
        self.to_y(k, block)
        self.to_x(k, block)
        self.to_partner(k, block)

    def from_xy(self, k, step):
        z = self.along_z(step)
        for ystep in range(1, self.ys):
            y = self.peer(self.y, ystep, self.ys)
            block = (self.x, z, y)
            self.arrived(k, block, self.y_sem.at[k, z * self.ys + y])
            for step in range(1, self.xs):
                device = self.device(self.peer(self.x, step, self.xs), self.c, self.z, self.y)
                self.send(k, 4, block, self.first, device, self.d_sem.at[k, self.x])
            self.to_partner(k, block)
        for xstep in range(1, self.xs):
            x = self.peer(self.x, xstep, self.xs)
            block = (x, z, self.y)
            self.arrived(k, block, self.x_sem.at[k, z * self.xs + x])
            for step in range(1, self.ys):
                device = self.device(self.x, self.c, self.z, self.peer(self.y, step, self.ys))
                self.send(k, 4, block, self.last, device, self.d_sem.at[k, x])
            self.to_partner(k, block)

    def from_diagonal(self, k):
        count = self.zs * (self.ys - 1)
        for xstep in range(1, self.xs):
            x = self.peer(self.x, xstep, self.xs)
            if count:
                region = self.buf.at[k, 0, pl.ds(0, count)]
                pltpu.make_async_copy(region, region, self.d_sem.at[k, x]).wait()
            for ystep in range(1, self.ys):
                for z in range(self.zs):
                    self.to_partner(k, (x, z, self.peer(self.y, ystep, self.ys)))

    def from_partner(self, k, x):
        region = self.buf.at[k, 0]
        pltpu.make_async_copy(region, region, self.p_sem.at[k, x]).wait()

    def all_left(self, k):
        xs, ys, zs = self.xs, self.ys, self.zs
        regions = [self.buf.at[k, pl.ds(0, xs)]]
        regions.append(self.buf.at[k, 0, pl.ds(0, zs - 1)] if zs > 1 else None)
        regions.append(self.buf.at[k, pl.ds(0, xs - 1), pl.ds(0, zs)] if xs > 1 else None)
        regions.append(self.buf.at[k, 0, pl.ds(0, zs * (ys - 1))] if ys > 1 else None)
        both = xs > 1 and ys > 1
        regions.append(self.buf.at[k, pl.ds(0, xs - 1), pl.ds(0, zs * (ys - 1))] if both else None)
        for kind, region in enumerate(regions):
            if region is not None:
                pltpu.make_async_copy(region, region, self.send_sem.at[k, kind]).wait()


class Exchange:
    def __init__(self, index, sent, landed, send_sem, recv_sem, peers, axis):
        self.sent, self.landed, self.peers, self.axis = sent, landed, peers, axis
        self.send_sem, self.recv_sem = send_sem.at[index], recv_sem.at[index]

    def start(self, me, source=None):
        for peer in self.peers:
            block = self.sent.at[peer[self.axis]] if source is None else source
            pltpu.make_async_remote_copy(
                src_ref=block,
                dst_ref=self.landed.at[me],
                send_sem=self.send_sem,
                recv_sem=self.recv_sem,
                device_id=peer,
                device_id_type=MESH,
            ).start()

    def region(self):
        return self.landed.at[pl.ds(0, len(self.peers))]

    def arrived(self):
        pltpu.make_async_copy(self.region(), self.region(), self.recv_sem).wait()

    def left(self):
        pltpu.make_async_copy(self.region(), self.region(), self.send_sem).wait()


def denoise_kernel(
    sizes, head_count, head_size,
    shift_ref, start_ref, label_ref, latent_ref, table_ref, w_patch_ref, w_final_ref, pos_ref, own_ref,
    class_hbm, w_freq_hbm, w_time_hbm, w_ada_hbm, latent_out, velocity_out,
    buf, tokens, normed, hidden, classes, w_freq, w_time, w_ada, features, window, sent_points, landed_points, sent_mod, landed_mod,
    sent_velocity, landed_velocity, sent_sums, landed_sums, anchors, rows_in,
    send_sem, z_sem, x_sem, y_sem, d_sem, p_sem, ex_send, ex_recv, ada_sem,
):
    steps, samples, lane_rows, lanes = latent_ref.shape
    patch_size, width = w_patch_ref.shape
    group = lanes // patch_size
    shards, blocks = sizes[0] * CORES, sizes[1] * sizes[2]
    own_samples = samples // blocks
    points = steps * own_samples
    block_rows, block_width = own_ref.shape[1:]
    columns = w_ada_hbm.shape[1]
    fetches = [
        pltpu.make_async_copy(source, target, ada_sem.at[i])
        for i, (source, target) in enumerate(
            [(w_freq_hbm, w_freq), (class_hbm, classes), (w_time_hbm, w_time), (w_ada_hbm, w_ada)]
        )
    ]
    for fetch in fetches:
        fetch.start()
    gather = Gather(sizes, own_ref, buf, send_sem, z_sem, x_sem, y_sem, d_sem, p_sem)
    tm, batch = gather.tm, gather.batch
    tm_peers, batch_peers = gather.tm_peers(), gather.batch_peers()
    ex = functools.partial(Exchange, send_sem=ex_send, recv_sem=ex_recv)
    latent_ex = ex(0, None, window, peers=tm_peers, axis="tm")
    mod_ex = ex(1, sent_mod, landed_mod, peers=tm_peers, axis="tm")
    point_ex = ex(2, sent_points, landed_points, peers=batch_peers, axis="batch")
    velocity_ex = ex(3, sent_velocity, landed_velocity, peers=batch_peers, axis="batch")
    sum_ex = ex(4, None, landed_sums, peers=tm_peers, axis="tm")
    gather.greet()
    window[tm] = latent_ref[...]
    for k in range(3):
        buf[k, tm, batch] = own_ref[k]
    gather.met()
    latent_ex.start(tm, latent_ref)
    gather.own_out(0)
    gather.to_z(0, range(1, sizes[2]))

    row_count = shards * points
    row_ids = lax.broadcasted_iota(jnp.int32, (row_count, classes.shape[0]), 0)
    class_ids = lax.broadcasted_iota(jnp.int32, (row_count, classes.shape[0]), 1)
    wanted = jnp.zeros_like(row_ids)
    for place in range(own_samples):
        sample = batch * own_samples + place
        wanted = jnp.where(row_ids % own_samples == place, label_ref[sample], wanted)
        for position in range(shards * steps):
            step_id = start_ref[sample] + shift_ref[sample] + position
            row = position * own_samples + place
            features[row : row + 1, :] = table_ref[pl.ds(step_id, 1), :]
    chosen = jnp.where(class_ids == wanted, 1.0, 0.0).astype(jnp.bfloat16)
    for fetch in fetches[:3]:
        fetch.wait()
    hidden_time = jnp.dot(
        features[...].astype(jnp.bfloat16), w_freq[...], preferred_element_type=jnp.float32
    )
    hidden_time = jax.nn.silu(hidden_time).astype(jnp.bfloat16)
    condition = jnp.dot(hidden_time, w_time[...], preferred_element_type=jnp.float32)
    condition = condition + jnp.dot(chosen, classes[...], preferred_element_type=jnp.float32)
    activation = jax.nn.silu(condition).astype(jnp.bfloat16)
    fetches[3].wait()
    mod = jnp.dot(activation, w_ada[...], preferred_element_type=jnp.float32)
    mod = mod.astype(jnp.bfloat16).astype(jnp.float32)
    for i in range(shards):
        sent_mod[i] = mod[i * points : (i + 1) * points]
    landed_mod[tm] = sent_mod[tm]
    mod_ex.start(tm)
    latent_ex.arrived()
    for sample in range(samples):
        shift = shift_ref[sample]
        anchors[sample] = window[shift // steps, shift % steps, sample]
        for step in range(steps):
            source = jnp.minimum(tm * steps + step + shift, shards * steps - 1)
            place = step * own_samples + sample % own_samples
            sent_points[sample // own_samples, place] = window[
                source // steps, source % steps, sample
            ]
    landed_points[batch] = sent_points[batch]
    point_ex.start(batch)
    for k in range(1, 3):
        gather.to_z(k, range(1, sizes[2]))

    def part(point, index):
        pieces, at = [], index * width
        while at < (index + 1) * width:
            start = at % columns
            size = min(columns - start, (index + 1) * width - at)
            pieces.append(landed_mod[at // columns, pl.ds(point, 1), start : start + size])
            at += size
        return pieces[0] if len(pieces) == 1 else jnp.concatenate(pieces, axis=1)

    def modulated(values, point, index):
        return (layer_norm(values) * (1.0 + part(point, index + 1)) + part(point, index)).astype(
            jnp.bfloat16
        )

    def enter(point, carry):
        for block in range(blocks):
            rows_in[block * lane_rows : (block + 1) * lane_rows, :] = landed_points[block, point]
        flat = rows_in[...].astype(jnp.bfloat16)
        pieces = [flat[:, k * patch_size : (k + 1) * patch_size] for k in range(group)]
        value = jnp.dot(
            jnp.concatenate(pieces, axis=0), w_patch_ref[...], preferred_element_type=jnp.float32
        )
        value = value + pos_ref[...]
        tokens[point] = value
        normed[point] = modulated(value, point, 0)
        return carry

    last = sizes[2] - 1
    for step in range(1, last):
        gather.from_z(0, step)
        gather.from_xy(0, step - 1)
    mod_ex.arrived()
    point_ex.arrived()
    lax.fori_loop(0, points // 2, enter, 0)
    if last:
        gather.from_z(0, last)
    lax.fori_loop(points // 2, points, enter, 0)
    for step in range(max(last - 1, 0), sizes[2]):
        gather.from_xy(0, step)
    gather.own_out(1)

    def weights(k, shard):
        return buf[k, shard].reshape(sizes[1] * sizes[2] * block_rows, block_width)

    def shard_of(turn):
        x = (gather.x + turn // CORES) % sizes[0]
        return x, x * CORES + (gather.c + turn % CORES) % CORES

    total_steps = shards * points

    def sweep(k, events, body):
        at = {}
        for share, event in events:
            at.setdefault(int(share * total_steps), []).append(event)

        def one(step, carry):
            turn, point = step // points, step % points
            x, shard = shard_of(turn)
            for when, todo in at.items():
                @pl.when(step == when)
                def _():
                    for event in todo:
                        event()

            @pl.when((point == 0) & (turn % CORES == 1))
            def _():
                gather.from_partner(k, x)

            body(shard, point)
            return carry

        lax.fori_loop(0, total_steps, one, 0)

    def relay(k, start, stop, last):
        todo = []
        zs = sizes[2]
        for step in range(1, zs):
            todo.append(functools.partial(gather.from_z, k, step))
            if step > 1:
                todo.append(functools.partial(gather.from_xy, k, step - 2))
        for step in range(max(zs - 2, 0), zs):
            todo.append(functools.partial(gather.from_xy, k, step))
        if last is not None:
            todo.append(functools.partial(gather.own_out, last))
        count = len(todo)
        return [(start + (stop - start) * i / max(count - 1, 1), e) for i, e in enumerate(todo)]

    def attention_step(shard, point):
        product = attention_product(normed[point], weights(0, shard), head_count, head_size)
        tokens[point] += part(point, 2) * product

    half = CORES / shards
    sweep(
        0,
        [(half, functools.partial(gather.from_diagonal, 0))] + relay(1, 0.1, 0.95, 2),
        attention_step,
    )

    def second(point, carry):
        normed[point] = modulated(tokens[point], point, 3)
        return carry

    lax.fori_loop(0, points, second, 0)

    def hidden_step(shard, point):
        value = jnp.dot(normed[point], weights(1, shard), preferred_element_type=jnp.float32)
        hidden[shard, point] = jax.nn.gelu(value, approximate=True).astype(jnp.bfloat16)

    sweep(
        1,
        [(half, functools.partial(gather.from_diagonal, 1))] + relay(2, 0.0, 0.95, None),
        hidden_step,
    )

    def residual_step(shard, point):
        product = times_transposed(hidden[shard, point], weights(2, shard))
        tokens[point] += part(point, 5) * product

    sweep(2, [(half, functools.partial(gather.from_diagonal, 2))], residual_step)

    def leave(point, carry):
        final_in = modulated(tokens[point], point, 6)
        value = times_transposed(final_in, w_final_ref[...])
        flat_rows = blocks * lane_rows
        pieces = [value[k * flat_rows : (k + 1) * flat_rows, :] for k in range(group)]
        flat = jnp.concatenate(pieces, axis=1).astype(jnp.bfloat16).astype(jnp.float32)
        for block in range(blocks):
            sent_velocity[block, point] = flat[block * lane_rows : (block + 1) * lane_rows]
        return carry

    lax.fori_loop(0, points, leave, 0)
    landed_velocity[batch] = sent_velocity[batch]
    velocity_ex.start(batch)
    velocity_ex.arrived()

    def step_velocity(step):
        value = landed_velocity[:, step * own_samples : (step + 1) * own_samples]
        return value.reshape(samples, lane_rows, lanes)

    total = step_velocity(0)
    for step in range(1, steps):
        total = total + step_velocity(step)
    sent_sums[...] = total
    sum_ex.start(tm, sent_sums)
    for step in range(steps):
        velocity_out[step] = step_velocity(step)
    sum_ex.arrived()
    running = jnp.zeros_like(total)
    for i in range(shards):
        running = running + jnp.where(i < tm, landed_sums[i], 0.0)
    for step in range(steps):
        latent_out[step] = anchors[...] + running * (1.0 / STEPS)
        running = running + step_velocity(step)
    for exchange in (latent_ex, mod_ex, point_ex, velocity_ex, sum_ex):
        exchange.left()
    for k in range(3):
        gather.all_left(k)


def denoise(sizes, whole, scalars, latents, w_patch, w_final, own, conditioning):
    steps, samples, lane_rows, lanes = latents.shape
    patch_size, width = w_patch.shape
    group = lanes // patch_size
    xs, ys, zs = sizes
    shards, blocks = xs * CORES, ys * zs
    token_count = blocks * lane_rows * group
    points = steps * samples // blocks
    block_rows, block_width = own.shape[1:]
    pos = jnp.asarray(position_table(token_count, group))
    dma = pltpu.SemaphoreType.DMA
    head_size = width // HEADS
    vmem = pl.BlockSpec(memory_space=pltpu.VMEM)
    smem = pl.BlockSpec(memory_space=pltpu.SMEM)
    result = jax.ShapeDtypeStruct(latents.shape, jnp.float32)
    pieces = pltpu.VMEM((blocks, points, lane_rows, lanes), jnp.float32)
    sums = (samples, lane_rows, lanes)
    columns = conditioning[-1].shape[1]
    mod = pltpu.VMEM((shards, points, columns), jnp.float32)
    table = jnp.asarray(step_table(whole))
    return pl.pallas_call(
        functools.partial(denoise_kernel, sizes, HEADS // shards, head_size),
        out_shape=(result, result),
        in_specs=[smem] * 3 + [vmem] * 6 + [pl.BlockSpec(memory_space=pl.ANY)] * 4,
        out_specs=(vmem, vmem),
        scratch_shapes=[
            pltpu.VMEM((3, shards, blocks, block_rows, block_width), jnp.bfloat16),
            pltpu.VMEM((points, token_count, width), jnp.float32),
            pltpu.VMEM((points, token_count, width), jnp.bfloat16),
            pltpu.VMEM((shards, points, token_count, block_width), jnp.bfloat16),
            *(pltpu.VMEM(value.shape, jnp.bfloat16) for value in conditioning),
            pltpu.VMEM((shards * points, FREQ), jnp.float32),
            pltpu.VMEM((shards, *latents.shape), jnp.float32),
            pieces,
            pieces,
            mod,
            mod,
            pieces,
            pieces,
            pltpu.VMEM(sums, jnp.float32),
            pltpu.VMEM((shards, *sums), jnp.float32),
            pltpu.VMEM(sums, jnp.float32),
            pltpu.VMEM((blocks * lane_rows, lanes), jnp.float32),
            dma((3, 5)),
            dma((3, zs)),
            dma((3, zs * xs)),
            dma((3, zs * ys)),
            dma((3, xs)),
            dma((3, xs)),
            dma((5,)),
            dma((5,)),
            dma((4,)),
        ],
        compiler_params=pltpu.CompilerParams(
            collective_id=0, has_side_effects=True, vmem_limit_bytes=67_000_000
        ),
        name="denoise",
    )(*scalars, latents, table, w_patch, w_final, pos, own, *conditioning)


def local(
    sizes,
    latents,
    shifts,
    starts,
    labels,
    class_table,
    w_freq,
    w_time,
    w_ada,
    w_patch,
    w_qkv,
    w_proj,
    w_fc1,
    w_fc2,
    w_final,
):
    local_steps, sample_total, lat_block = latents.shape
    own = jnp.stack([jnp.concatenate([w_qkv, w_proj.T], axis=1), w_fc1, w_fc2.T])
    rows = latents.reshape(local_steps, sample_total, lat_block // LANES, LANES)
    scalars = (shifts, starts, labels)
    conditioning = (class_table, w_freq, w_time, w_ada)
    whole = STEPS + 2 * local_steps * lax.axis_size("tm")
    latents_out, velocity = denoise(
        sizes, whole, scalars, rows, w_patch, w_final.T, own, conditioning
    )
    return (
        latents_out.reshape(latents.shape),
        velocity.astype(jnp.bfloat16).reshape(latents.shape),
    )


def chip_sizes(mesh):
    batch = mesh.shape["batch"]
    ys = 1
    while ys * ys * 4 <= batch:
        ys *= 2
    return mesh.shape["tm"] // CORES, ys, batch // ys


def solution(mesh):
    placed = (
        P("tm", None, "batch"),
        P(),
        P(),
        P(),
        P(),
        P(),
        P(),
        P(None, "tm"),
        P(),
        P("batch", "tm"),
        P("tm", "batch"),
        P("batch", "tm"),
        P("tm", "batch"),
        P(),
    )
    return jax.shard_map(
        functools.partial(local, chip_sizes(mesh)),
        mesh=mesh,
        in_specs=placed,
        out_specs=(P("tm", None, "batch"), P("tm", None, "batch")),
        check_vma=False,
    )
```

```python
import functools
import math

import jax
import jax.numpy as jnp
import numpy as np
from jax import lax
from jax.experimental import pallas as pl
from jax.experimental.pallas import tpu as pltpu
from jax.sharding import PartitionSpec as P

D = 1152
HEADS = 16
FREQ = 256
GRID = 16
STEPS = 18
LANES = 128
CORES = 2
MESH = pl.DeviceIdType.MESH


def layer_norm(values):
    average = jnp.mean(values, axis=-1, keepdims=True)
    centred = values - average
    variance = jnp.mean(centred * centred, axis=-1, keepdims=True)
    return centred * lax.rsqrt(variance + 1e-06)


def position_table(token_count, group):
    token_ids = np.arange(token_count).reshape(token_count // group, group).T.reshape(-1)
    row_ids = (token_ids // GRID).astype(np.float32)
    col_ids = (token_ids % GRID).astype(np.float32)
    quarter = D // 4
    omegas = np.exp(-math.log(10000.0) * np.arange(quarter, dtype=np.float32) / quarter).astype(np.float32)
    col_angle = col_ids[:, None] * omegas[None, :]
    row_angle = row_ids[:, None] * omegas[None, :]
    return np.concatenate(
        [np.sin(col_angle), np.cos(col_angle), np.sin(row_angle), np.cos(row_angle)], axis=1
    ).astype(np.float32)

def step_table(count):
    half_freq = FREQ // 2
    freqs = np.exp(-math.log(10000.0) * np.arange(half_freq, dtype=np.float32) / half_freq)
    tvalue = 1000.0 * (1.0 - np.arange(count, dtype=np.float32) / np.float32(STEPS))
    angles = tvalue.astype(np.float32)[:, None] * freqs.astype(np.float32)[None, :]
    return np.concatenate([np.cos(angles), np.sin(angles)], axis=1).astype(np.float32)


def times_transposed(left, right):
    return lax.dot_general(
        left, right, (((1,), (1,)), ((), ())), preferred_element_type=jnp.float32
    )


def attention_product(rows_in, entry, head_count, head_size):
    qkv_width = 3 * head_count * head_size
    boundary = qkv_width // LANES * LANES
    rows = jnp.dot(rows_in, entry[:, :qkv_width], preferred_element_type=jnp.float32)
    rows = rows.astype(jnp.bfloat16)
    scale = 1.0 / math.sqrt(head_size)
    pieces = []
    if qkv_width > boundary:
        pieces.append(jnp.zeros((rows.shape[0], qkv_width - boundary), jnp.bfloat16))
    for head in range(head_count):
        start = head * 3 * head_size
        query = rows[:, start : start + head_size]
        keys = rows[:, start + head_size : start + 2 * head_size]
        values = rows[:, start + 2 * head_size : start + 3 * head_size]
        scores = times_transposed(query, keys)
        peak = jnp.max(scores, axis=-1, keepdims=True)
        weights = jnp.exp((scores - peak) * scale)
        total = jnp.sum(weights, axis=-1, keepdims=True)
        mixed = jnp.dot(
            weights.astype(jnp.bfloat16), values, preferred_element_type=jnp.float32
        )
        pieces.append((mixed / total).astype(jnp.bfloat16))
    attended = jnp.concatenate(pieces, axis=1)
    return times_transposed(attended, entry[:, boundary:])


class Gather:
    def __init__(self, sizes, own, buf, send_sem, z_sem, x_sem, y_sem, d_sem, p_sem):
        self.xs, self.ys, self.zs = sizes
        self.own, self.buf = own, buf
        self.send_sem, self.z_sem, self.x_sem = send_sem, z_sem, x_sem
        self.y_sem, self.d_sem, self.p_sem = y_sem, d_sem, p_sem
        tm, batch = lax.axis_index("tm"), lax.axis_index("batch")
        self.x, self.c = tm // CORES, tm % CORES
        self.z, self.y = batch // self.ys, batch % self.ys
        self.tm, self.batch = tm, batch
        rows = own.shape[1]
        self.cut = (rows // 32) * 16
        self.whole = pl.ds(0, rows)
        self.first = pl.ds(0, rows - self.cut)
        self.last = pl.ds(rows - self.cut, self.cut)

    def peer(self, position, step, size):
        return (position + step) % size

    def along_z(self, step):
        direction = 1 - 2 * (self.z * 2 // self.zs)
        return (self.z + direction * step + self.zs) % self.zs

    def device(self, x, c, z, y):
        return {"tm": x * CORES + c, "batch": z * self.ys + y}

    def tm_peers(self):
        count = self.xs * CORES
        return [{"tm": (self.tm + i) % count, "batch": self.batch} for i in range(1, count)]

    def batch_peers(self):
        count = self.ys * self.zs
        return [{"tm": self.tm, "batch": (self.batch + i) % count} for i in range(1, count)]

    def peers(self):
        return self.tm_peers() + self.batch_peers()

    def greet(self):
        barrier = pltpu.get_barrier_semaphore()
        for device in self.peers():
            pl.semaphore_signal(barrier, inc=1, device_id=device, device_id_type=MESH)

    def met(self):
        pl.semaphore_wait(pltpu.get_barrier_semaphore(), len(self.peers()))

    def place(self, k, x, z, y, rows):
        return self.buf.at[k, x * CORES + self.c, z * self.ys + y, rows]

    def send(self, k, kind, block, rows, device, arrival, own=False):
        target = self.place(k, *block, rows)
        source = self.own.at[k, rows] if own else target
        pltpu.make_async_remote_copy(
            src_ref=source,
            dst_ref=target,
            send_sem=self.send_sem.at[k, kind],
            recv_sem=arrival,
            device_id=device,
            device_id_type=MESH,
        ).start()

    def arrived(self, k, block, arrival):
        region = self.place(k, *block, self.whole)
        pltpu.make_async_copy(region, region, arrival).wait()

    def to_partner(self, k, block, own=False):
        device = self.device(self.x, 1 - self.c, self.z, self.y)
        self.send(k, 0, block, self.whole, device, self.p_sem.at[k, block[0]], own)

    def to_z(self, k, steps):
        block = (self.x, self.z, self.y)
        for step in steps:
            device = self.device(self.x, self.c, self.along_z(step), self.y)
            self.send(k, 1, block, self.whole, device, self.z_sem.at[k, self.z], True)

    def to_x(self, k, block, own=False):
        for step in range(1, self.xs):
            device = self.device(self.peer(self.x, step, self.xs), self.c, self.z, self.y)
            arrival = self.x_sem.at[k, block[1] * self.xs + self.x]
            self.send(k, 2, block, self.whole, device, arrival, own)

    def to_y(self, k, block, own=False):
        for step in range(1, self.ys):
            device = self.device(self.x, self.c, self.z, self.peer(self.y, step, self.ys))
            arrival = self.y_sem.at[k, block[1] * self.ys + self.y]
            self.send(k, 3, block, self.whole, device, arrival, own)

    def own_out(self, k):
        block = (self.x, self.z, self.y)
        self.to_y(k, block, True)
        self.to_x(k, block, True)
        self.to_partner(k, block, True)

    def from_z(self, k, step):
        z = self.along_z(step)
        block = (self.x, z, self.y)
        self.arrived(k, block, self.z_sem.at[k, z])
        self.to_y(k, block)
        self.to_x(k, block)
        self.to_partner(k, block)

    def from_xy(self, k, step):
        z = self.along_z(step)
        for ystep in range(1, self.ys):
            y = self.peer(self.y, ystep, self.ys)
            block = (self.x, z, y)
            self.arrived(k, block, self.y_sem.at[k, z * self.ys + y])
            for step in range(1, self.xs):
                device = self.device(self.peer(self.x, step, self.xs), self.c, self.z, self.y)
                self.send(k, 4, block, self.first, device, self.d_sem.at[k, self.x])
            self.to_partner(k, block)
        for xstep in range(1, self.xs):
            x = self.peer(self.x, xstep, self.xs)
            block = (x, z, self.y)
            self.arrived(k, block, self.x_sem.at[k, z * self.xs + x])
            for step in range(1, self.ys):
                device = self.device(self.x, self.c, self.z, self.peer(self.y, step, self.ys))
                self.send(k, 4, block, self.last, device, self.d_sem.at[k, x])
            self.to_partner(k, block)

    def from_diagonal(self, k):
        count = self.zs * (self.ys - 1)
        for xstep in range(1, self.xs):
            x = self.peer(self.x, xstep, self.xs)
            if count:
                region = self.buf.at[k, 0, pl.ds(0, count)]
                pltpu.make_async_copy(region, region, self.d_sem.at[k, x]).wait()
            for ystep in range(1, self.ys):
                for z in range(self.zs):
                    self.to_partner(k, (x, z, self.peer(self.y, ystep, self.ys)))

    def from_partner(self, k, x):
        region = self.buf.at[k, 0]
        pltpu.make_async_copy(region, region, self.p_sem.at[k, x]).wait()

    def all_left(self, k):
        xs, ys, zs = self.xs, self.ys, self.zs
        regions = [self.buf.at[k, pl.ds(0, xs)]]
        regions.append(self.buf.at[k, 0, pl.ds(0, zs - 1)] if zs > 1 else None)
        regions.append(self.buf.at[k, pl.ds(0, xs - 1), pl.ds(0, zs)] if xs > 1 else None)
        regions.append(self.buf.at[k, 0, pl.ds(0, zs * (ys - 1))] if ys > 1 else None)
        both = xs > 1 and ys > 1
        regions.append(self.buf.at[k, pl.ds(0, xs - 1), pl.ds(0, zs * (ys - 1))] if both else None)
        for kind, region in enumerate(regions):
            if region is not None:
                pltpu.make_async_copy(region, region, self.send_sem.at[k, kind]).wait()


class Exchange:
    def __init__(self, index, sent, landed, send_sem, recv_sem, peers, axis):
        self.sent, self.landed, self.peers, self.axis = sent, landed, peers, axis
        self.send_sem, self.recv_sem = send_sem.at[index], recv_sem.at[index]

    def start(self, me, source=None):
        for peer in self.peers:
            block = self.sent.at[peer[self.axis]] if source is None else source
            pltpu.make_async_remote_copy(
                src_ref=block,
                dst_ref=self.landed.at[me],
                send_sem=self.send_sem,
                recv_sem=self.recv_sem,
                device_id=peer,
                device_id_type=MESH,
            ).start()

    def region(self):
        return self.landed.at[pl.ds(0, len(self.peers))]

    def arrived(self):
        pltpu.make_async_copy(self.region(), self.region(), self.recv_sem).wait()

    def left(self):
        pltpu.make_async_copy(self.region(), self.region(), self.send_sem).wait()


def denoise_kernel(
    sizes, head_count, head_size,
    shift_ref, start_ref, label_ref, latent_ref, table_ref, w_patch_ref, w_final_ref, pos_ref, own_ref,
    class_hbm, w_freq_hbm, w_time_hbm, w_ada_hbm, latent_out, velocity_out,
    buf, tokens, normed, hidden, classes, w_freq, w_time, w_ada, features, window, sent_points, landed_points, sent_mod, landed_mod,
    sent_velocity, landed_velocity, sent_sums, landed_sums, anchors, rows_in,
    send_sem, z_sem, x_sem, y_sem, d_sem, p_sem, ex_send, ex_recv, ada_sem,
):
    steps, samples, lane_rows, lanes = latent_ref.shape
    patch_size, width = w_patch_ref.shape
    group = lanes // patch_size
    shards, blocks = sizes[0] * CORES, sizes[1] * sizes[2]
    own_samples = samples // blocks
    points = steps * own_samples
    block_rows, block_width = own_ref.shape[1:]
    columns = w_ada_hbm.shape[1]
    fetches = [
        pltpu.make_async_copy(source, target, ada_sem.at[i])
        for i, (source, target) in enumerate(
            [(w_freq_hbm, w_freq), (class_hbm, classes), (w_time_hbm, w_time), (w_ada_hbm, w_ada)]
        )
    ]
    for fetch in fetches:
        fetch.start()
    gather = Gather(sizes, own_ref, buf, send_sem, z_sem, x_sem, y_sem, d_sem, p_sem)
    tm, batch = gather.tm, gather.batch
    tm_peers, batch_peers = gather.tm_peers(), gather.batch_peers()
    ex = functools.partial(Exchange, send_sem=ex_send, recv_sem=ex_recv)
    latent_ex = ex(0, None, window, peers=tm_peers, axis="tm")
    mod_ex = ex(1, sent_mod, landed_mod, peers=tm_peers, axis="tm")
    point_ex = ex(2, sent_points, landed_points, peers=batch_peers, axis="batch")
    velocity_ex = ex(3, sent_velocity, landed_velocity, peers=batch_peers, axis="batch")
    sum_ex = ex(4, None, landed_sums, peers=tm_peers, axis="tm")
    gather.greet()
    window[tm] = latent_ref[...]
    for k in range(3):
        buf[k, tm, batch] = own_ref[k]
    gather.met()
    latent_ex.start(tm, latent_ref)
    gather.own_out(0)
    gather.to_z(0, range(1, sizes[2]))

    row_count = shards * points
    row_ids = lax.broadcasted_iota(jnp.int32, (row_count, classes.shape[0]), 0)
    class_ids = lax.broadcasted_iota(jnp.int32, (row_count, classes.shape[0]), 1)
    wanted = jnp.zeros_like(row_ids)
    for place in range(own_samples):
        sample = batch * own_samples + place
        wanted = jnp.where(row_ids % own_samples == place, label_ref[sample], wanted)
        for position in range(shards * steps):
            step_id = start_ref[sample] + shift_ref[sample] + position
            row = position * own_samples + place
            features[row : row + 1, :] = table_ref[pl.ds(step_id, 1), :]
    chosen = jnp.where(class_ids == wanted, 1.0, 0.0).astype(jnp.bfloat16)
    for fetch in fetches[:3]:
        fetch.wait()
    hidden_time = jnp.dot(
        features[...].astype(jnp.bfloat16), w_freq[...], preferred_element_type=jnp.float32
    )
    hidden_time = jax.nn.silu(hidden_time).astype(jnp.bfloat16)
    condition = jnp.dot(hidden_time, w_time[...], preferred_element_type=jnp.float32)
    condition = condition + jnp.dot(chosen, classes[...], preferred_element_type=jnp.float32)
    activation = jax.nn.silu(condition).astype(jnp.bfloat16)
    fetches[3].wait()
    mod = jnp.dot(activation, w_ada[...], preferred_element_type=jnp.float32)
    mod = mod.astype(jnp.bfloat16).astype(jnp.float32)
    for i in range(shards):
        sent_mod[i] = mod[i * points : (i + 1) * points]
    landed_mod[tm] = sent_mod[tm]
    mod_ex.start(tm)
    latent_ex.arrived()
    for sample in range(samples):
        shift = shift_ref[sample]
        anchors[sample] = window[shift // steps, shift % steps, sample]
        for step in range(steps):
            source = jnp.minimum(tm * steps + step + shift, shards * steps - 1)
            place = step * own_samples + sample % own_samples
            sent_points[sample // own_samples, place] = window[
                source // steps, source % steps, sample
            ]
    landed_points[batch] = sent_points[batch]
    point_ex.start(batch)
    for k in range(1, 3):
        gather.to_z(k, range(1, sizes[2]))

    def part(point, index):
        pieces, at = [], index * width
        while at < (index + 1) * width:
            start = at % columns
            size = min(columns - start, (index + 1) * width - at)
            pieces.append(landed_mod[at // columns, pl.ds(point, 1), start : start + size])
            at += size
        return pieces[0] if len(pieces) == 1 else jnp.concatenate(pieces, axis=1)

    def modulated(values, point, index):
        return (layer_norm(values) * (1.0 + part(point, index + 1)) + part(point, index)).astype(
            jnp.bfloat16
        )

    def enter(point, carry):
        for block in range(blocks):
            rows_in[block * lane_rows : (block + 1) * lane_rows, :] = landed_points[block, point]
        flat = rows_in[...].astype(jnp.bfloat16)
        pieces = [flat[:, k * patch_size : (k + 1) * patch_size] for k in range(group)]
        value = jnp.dot(
            jnp.concatenate(pieces, axis=0), w_patch_ref[...], preferred_element_type=jnp.float32
        )
        value = value + pos_ref[...]
        tokens[point] = value
        normed[point] = modulated(value, point, 0)
        return carry

    last = sizes[2] - 1
    for step in range(1, last):
        gather.from_z(0, step)
        gather.from_xy(0, step - 1)
    mod_ex.arrived()
    point_ex.arrived()
    lax.fori_loop(0, points // 2, enter, 0)
    if last:
        gather.from_z(0, last)
    lax.fori_loop(points // 2, points, enter, 0)
    for step in range(max(last - 1, 0), sizes[2]):
        if step == last:
            gather.own_out(1)
        gather.from_xy(0, step)

    def weights(k, shard):
        return buf[k, shard].reshape(sizes[1] * sizes[2] * block_rows, block_width)

    def shard_of(turn):
        x = (gather.x + turn // CORES) % sizes[0]
        return x, x * CORES + (gather.c + turn % CORES) % CORES

    def sweep(k, events, body, together=1):
        turns = points // together
        total_steps = shards * turns
        at = {}
        for share, event in events:
            at.setdefault(int(share * total_steps), []).append(event)

        def one(step, carry):
            turn, point = step // turns, step % turns * together
            x, shard = shard_of(turn)
            for when, todo in at.items():
                @pl.when(step == when)
                def _():
                    for event in todo:
                        event()

            @pl.when((point == 0) & (turn % CORES == 1))
            def _():
                gather.from_partner(k, x)

            body(shard, point)
            return carry

        lax.fori_loop(0, total_steps, one, 0)

    def relay(k, start, stop, last):
        todo = []
        zs = sizes[2]
        for step in range(1, zs):
            todo.append(functools.partial(gather.from_z, k, step))
            if step > 1:
                todo.append(functools.partial(gather.from_xy, k, step - 2))
        for step in range(max(zs - 2, 0), zs):
            if last is not None and step == zs - 1:
                todo.append(functools.partial(gather.own_out, last))
            todo.append(functools.partial(gather.from_xy, k, step))
        count = len(todo)
        return [(start + (stop - start) * i / max(count - 1, 1), e) for i, e in enumerate(todo)]

    def attention_step(shard, point):
        product = attention_product(normed[point], weights(0, shard), head_count, head_size)
        tokens[point] += part(point, 2) * product

    half = CORES / shards
    sweep(
        0,
        [(half, functools.partial(gather.from_diagonal, 0))] + relay(1, 0.06, 0.75, 2),
        attention_step,
    )

    def second(point, carry):
        normed[point] = modulated(tokens[point], point, 3)
        return carry

    lax.fori_loop(0, points, second, 0)

    def hidden_step(shard, point):
        value = jnp.dot(normed[point], weights(1, shard), preferred_element_type=jnp.float32)
        hidden[shard, point] = jax.nn.gelu(value, approximate=True).astype(jnp.bfloat16)

    sweep(
        1,
        [(half, functools.partial(gather.from_diagonal, 1))] + relay(2, 0.0, 0.95, None),
        hidden_step,
    )

    together = 2 - points % 2

    def residual_step(shard, point):
        units = hidden[shard, pl.ds(point, together)]
        count, token_count = units.shape[:2]
        units = units.reshape(count * token_count, block_width)
        product = times_transposed(units, weights(2, shard))
        for i in range(count):
            rows = product[i * token_count : (i + 1) * token_count]
            tokens[point + i] += part(point + i, 5) * rows

    last_events = [(half, functools.partial(gather.from_diagonal, 2))]
    sweep(2, last_events, residual_step, together)

    def leave(point, carry):
        final_in = modulated(tokens[point], point, 6)
        value = times_transposed(final_in, w_final_ref[...])
        flat_rows = blocks * lane_rows
        pieces = [value[k * flat_rows : (k + 1) * flat_rows, :] for k in range(group)]
        flat = jnp.concatenate(pieces, axis=1).astype(jnp.bfloat16).astype(jnp.float32)
        for block in range(blocks):
            sent_velocity[block, point] = flat[block * lane_rows : (block + 1) * lane_rows]
        return carry

    lax.fori_loop(0, points, leave, 0)
    landed_velocity[batch] = sent_velocity[batch]
    velocity_ex.start(batch)
    velocity_ex.arrived()

    def step_velocity(step):
        value = landed_velocity[:, step * own_samples : (step + 1) * own_samples]
        return value.reshape(samples, lane_rows, lanes)

    total = step_velocity(0)
    for step in range(1, steps):
        total = total + step_velocity(step)
    sent_sums[...] = total
    sum_ex.start(tm, sent_sums)
    for step in range(steps):
        velocity_out[step] = step_velocity(step)
    sum_ex.arrived()
    running = jnp.zeros_like(total)
    for i in range(shards):
        running = running + jnp.where(i < tm, landed_sums[i], 0.0)
    for step in range(steps):
        latent_out[step] = anchors[...] + running * (1.0 / STEPS)
        running = running + step_velocity(step)
    for exchange in (latent_ex, mod_ex, point_ex, velocity_ex, sum_ex):
        exchange.left()
    for k in range(3):
        gather.all_left(k)


def denoise(sizes, whole, scalars, latents, w_patch, w_final, own, conditioning):
    steps, samples, lane_rows, lanes = latents.shape
    patch_size, width = w_patch.shape
    group = lanes // patch_size
    xs, ys, zs = sizes
    shards, blocks = xs * CORES, ys * zs
    token_count = blocks * lane_rows * group
    points = steps * samples // blocks
    block_rows, block_width = own.shape[1:]
    pos = jnp.asarray(position_table(token_count, group))
    dma = pltpu.SemaphoreType.DMA
    head_size = width // HEADS
    vmem = pl.BlockSpec(memory_space=pltpu.VMEM)
    smem = pl.BlockSpec(memory_space=pltpu.SMEM)
    result = jax.ShapeDtypeStruct(latents.shape, jnp.float32)
    pieces = pltpu.VMEM((blocks, points, lane_rows, lanes), jnp.float32)
    sums = (samples, lane_rows, lanes)
    columns = conditioning[-1].shape[1]
    mod = pltpu.VMEM((shards, points, columns), jnp.float32)
    table = jnp.asarray(step_table(whole))
    return pl.pallas_call(
        functools.partial(denoise_kernel, sizes, HEADS // shards, head_size),
        out_shape=(result, result),
        in_specs=[smem] * 3 + [vmem] * 6 + [pl.BlockSpec(memory_space=pl.ANY)] * 4,
        out_specs=(vmem, vmem),
        scratch_shapes=[
            pltpu.VMEM((3, shards, blocks, block_rows, block_width), jnp.bfloat16),
            pltpu.VMEM((points, token_count, width), jnp.float32),
            pltpu.VMEM((points, token_count, width), jnp.bfloat16),
            pltpu.VMEM((shards, points, token_count, block_width), jnp.bfloat16),
            *(pltpu.VMEM(value.shape, jnp.bfloat16) for value in conditioning),
            pltpu.VMEM((shards * points, FREQ), jnp.float32),
            pltpu.VMEM((shards, *latents.shape), jnp.float32),
            pieces,
            pieces,
            mod,
            mod,
            pieces,
            pieces,
            pltpu.VMEM(sums, jnp.float32),
            pltpu.VMEM((shards, *sums), jnp.float32),
            pltpu.VMEM(sums, jnp.float32),
            pltpu.VMEM((blocks * lane_rows, lanes), jnp.float32),
            dma((3, 5)),
            dma((3, zs)),
            dma((3, zs * xs)),
            dma((3, zs * ys)),
            dma((3, xs)),
            dma((3, xs)),
            dma((5,)),
            dma((5,)),
            dma((4,)),
        ],
        compiler_params=pltpu.CompilerParams(
            collective_id=0, has_side_effects=True, vmem_limit_bytes=67_000_000
        ),
        name="denoise",
    )(*scalars, latents, table, w_patch, w_final, pos, own, *conditioning)


def local(
    sizes,
    latents,
    shifts,
    starts,
    labels,
    class_table,
    w_freq,
    w_time,
    w_ada,
    w_patch,
    w_qkv,
    w_proj,
    w_fc1,
    w_fc2,
    w_final,
):
    local_steps, sample_total, lat_block = latents.shape
    own = jnp.stack([jnp.concatenate([w_qkv, w_proj.T], axis=1), w_fc1, w_fc2.T])
    rows = latents.reshape(local_steps, sample_total, lat_block // LANES, LANES)
    scalars = (shifts, starts, labels)
    conditioning = (class_table, w_freq, w_time, w_ada)
    whole = STEPS + 2 * local_steps * lax.axis_size("tm")
    latents_out, velocity = denoise(
        sizes, whole, scalars, rows, w_patch, w_final.T, own, conditioning
    )
    return (
        latents_out.reshape(latents.shape),
        velocity.astype(jnp.bfloat16).reshape(latents.shape),
    )


def chip_sizes(mesh):
    batch = mesh.shape["batch"]
    ys = 1
    while ys * ys * 4 <= batch:
        ys *= 2
    return mesh.shape["tm"] // CORES, ys, batch // ys


def solution(mesh):
    placed = (
        P("tm", None, "batch"),
        P(),
        P(),
        P(),
        P(),
        P(),
        P(),
        P(None, "tm"),
        P(),
        P("batch", "tm"),
        P("tm", "batch"),
        P("batch", "tm"),
        P("tm", "batch"),
        P(),
    )
    return jax.shard_map(
        functools.partial(local, chip_sizes(mesh)),
        mesh=mesh,
        in_specs=placed,
        out_specs=(P("tm", None, "batch"), P("tm", None, "batch")),
        check_vma=False,
    )
```
